256 devices in a mesh: dp: 32 (over y, x, core), section: 8 (over z).
Axes of the slice: x: 4, y: 4, z: 8, core: 2. Of those that a mesh axis runs over, the one named last changes fastest.
Arguments:
- activations: bfloat16 [4, 2048, 2048], P(None, 'dp'), may hold values from -6 to 6
- cotangent: bfloat16 [4, 2048, 2048], P(None, 'dp'), may hold values from -6 to 6
- weight: bfloat16 [8, 2048, 2048], P('section', 'dp'), may hold values from -0.125 to 0.125
- norm_gain: float32 [8, 2048], P('section'), may hold values from 0.1 to 1.9
- pair_mask: int32 [8, 512, 2048], P('section'), may hold values from 0 to 5, as said below
- earlier_mask: int32 [8, 512, 2048], P('section', 'dp'), may hold values from 0 to 5, as said below
Outputs:
- weight_grad: float32 [8, 2048, 2048], P('section', 'dp')
- flip_count: int32 [8], P('section')
The draws below stay inside these ranges and needn't reach their ends.
Inputs may be any that keep to these rules, and one draw needn't show every extreme that they name: `pair_mask`: pair number of each group of four consecutive rows and each column; pairs numbered (0,1), (0,2), (0,3), (1,2), (1,3), (2,3). `earlier_mask`: pair numbers of the previous step, numbered likewise.
All inputs are finite; a program needn't handle non-finite values.
Results may differ from the reference program's by a relative error of at most 0.02.
Values may be sent and summed in bfloat16 or wider, within the bound.
A program may use at most 64 MiB of HBM per device.

```python
import math
import jax
import jax.numpy as jnp
from jax import lax

D = 2048
MICRO = 4
SECTIONS = 8
BATCH_ROWS = 2048
TOKENS = 8192
N_DP = 32


def mask_pair(key):
    base_key = jax.random.fold_in(key, 7301)
    mask_shape = (SECTIONS, D // 4, D)
    current = jax.random.randint(jax.random.fold_in(base_key, 1), mask_shape, 0, 6)
    row_iota = lax.broadcasted_iota(jnp.int32, mask_shape, 1)
    threshold = 100 + 200 * row_iota // (D // 4 - 1)
    dice_rolls = jax.random.randint(jax.random.fold_in(base_key, 2), mask_shape, 0, 1000)
    offsets = jax.random.randint(jax.random.fold_in(base_key, 3), mask_shape, 1, 6)
    earlier = jnp.where(dice_rolls < threshold, (current + offsets) % 6, current)
    return (current.astype(jnp.int32), earlier.astype(jnp.int32))


def draw_pair_mask(key, part):
    return mask_pair(key)[0]


def draw_earlier_mask(key, part):
    return mask_pair(key)[1]


def levels(rng, shape, cuts, smallest, high):
    gain, own = 1.0, jax.random.fold_in(rng, 6)
    for position, blocks in cuts:
        steps = jnp.exp(jax.random.uniform(jax.random.fold_in(own, position), (blocks,), jnp.float32, smallest / len(cuts), high / len(cuts)))
        gain = gain * jnp.repeat(steps, shape[position] // blocks).reshape([-1 if axis == position else 1 for axis in range(len(shape))])
    return gain


def centred(key, extent, width, most, cuts=(), kind=jnp.bfloat16):
    loudness = levels(key, extent, cuts, -0.22, 0.18) if cuts else 1.0
    result = jax.random.normal(key, extent, jnp.float32) * width * loudness
    return jnp.minimum(jnp.maximum(result, -most), most).astype(kind)


def setup_inputs(seed: int = 0) -> dict:
    key_of = jax.random.split(jax.random.key(seed), 7)
    activations = centred(key_of[0], (MICRO, BATCH_ROWS, D), 1.0, 6.0, ((1, 32),))
    cotangent = centred(key_of[1], (MICRO, BATCH_ROWS, D), 1.0, 6.0, ((1, 32),))
    weight = centred(key_of[2], (SECTIONS, D, D), D ** -0.5, 0.125, ((0, 8), (1, 32)))
    norm_gain = jnp.clip(1.0 + 0.18 * jax.random.normal(key_of[3], (SECTIONS, D), jnp.float32), 0.1, 1.9)
    pair_mask = draw_pair_mask(jax.random.fold_in(key_of[6], 71), 0)
    earlier_mask = draw_earlier_mask(jax.random.fold_in(key_of[6], 71), 0)
    return {"activations": activations, "cotangent": cotangent, "weight": weight, "norm_gain": norm_gain, "pair_mask": pair_mask, "earlier_mask": earlier_mask}


epsilon = 1e-06
decay_rate = 4.0
half_root = 0.7071067811865476
density_scale = 0.3989422804014327
first_table = (0, 0, 0, 1, 1, 2)
second_table = (1, 2, 3, 2, 3, 3)

def pair_ends(indices):
    leading = jnp.zeros_like(indices)
    trailing = jnp.zeros_like(indices)
    for pair_index in range(6):
        matches = indices == pair_index
        leading = jnp.where(matches, first_table[pair_index], leading)
        trailing = jnp.where(matches, second_table[pair_index], trailing)
    return (leading, trailing)

def kept_positions(indices):
    leading, trailing = pair_ends(indices)
    groups, columns = indices.shape
    positions = lax.broadcasted_iota(jnp.int32, (groups, 4, columns), 1)
    kept_mask = (positions == leading[:, None, :]) | (positions == trailing[:, None, :])
    return kept_mask.reshape(groups * 4, columns)

def section_forward(inputs, masked, gain_row):
    values = inputs.astype(jnp.float32)
    norm_scale = lax.rsqrt(lax.optimization_barrier(jnp.mean(values * values, axis=-1, keepdims=True)) + epsilon)
    normed = (values * norm_scale * gain_row).astype(jnp.bfloat16)
    preact = jnp.dot(normed, masked, preferred_element_type=jnp.float32)
    normal_cdf = 0.5 * (1.0 + lax.erf(preact * half_root))
    outputs = (values + preact * normal_cdf).astype(jnp.bfloat16)
    return (normed, preact, outputs)

def section_backward(inputs, preact, upstream, masked, gain_row):
    values = inputs.astype(jnp.float32)
    norm_scale = lax.rsqrt(lax.optimization_barrier(jnp.mean(values * values, axis=-1, keepdims=True)) + epsilon)
    normal_cdf = 0.5 * (1.0 + lax.erf(preact * half_root))
    normal_pdf = jnp.exp(-0.5 * preact * preact) * density_scale
    upstream_f = upstream.astype(jnp.float32)
    grad_pre = (upstream_f * (normal_cdf + preact * normal_pdf)).astype(jnp.bfloat16)
    grad_normed = lax.dot_general(grad_pre, masked, (((1,), (1,)), ((), ())), preferred_element_type=jnp.float32)
    scaled_grad = grad_normed * gain_row
    grad_input = norm_scale * scaled_grad - values * norm_scale ** 3 * lax.optimization_barrier(jnp.mean(scaled_grad * values, axis=-1, keepdims=True))
    return (grad_pre, (upstream_f + grad_input).astype(jnp.bfloat16))

def replica_terms(normed, grad_pre, micro_count):
    replicas = N_DP
    model_width = normed.shape[1]
    row_count = normed.shape[0] // (micro_count * replicas)
    normed_split = normed.reshape(micro_count, replicas, row_count, model_width).transpose(1, 0, 2, 3).reshape(replicas, micro_count * row_count, model_width)
    grad_split = grad_pre.reshape(micro_count, replicas, row_count, model_width).transpose(1, 0, 2, 3).reshape(replicas, micro_count * row_count, model_width)

    def add_replica(running, pieces):
        partial_term = lax.dot_general(pieces[0], pieces[1], (((0,), (0,)), ((), ())), preferred_element_type=jnp.float32)
        rounded = lax.optimization_barrier(partial_term.astype(jnp.bfloat16))
        return (running + rounded.astype(jnp.float32), None)
    running, unused = lax.scan(add_replica, jnp.zeros((model_width, model_width), jnp.float32), (normed_split, grad_split))
    return running

def reference(activations, cotangent, weight, norm_gain, pair_mask, earlier_mask):
    micro_count, batch_rows, model_width = activations.shape
    hidden = activations.reshape(micro_count * batch_rows, model_width)
    upstream = cotangent.reshape(micro_count * batch_rows, model_width)
    masked_list = []
    kept_list = []
    for section_index in range(SECTIONS):
        kept_mask = kept_positions(pair_mask[section_index])
        kept_list.append(kept_mask)
        masked_list.append(jnp.where(kept_mask, weight[section_index], jnp.zeros_like(weight[section_index])))
    saved_inputs = []
    saved_normed = []
    saved_preact = []
    for section_index in range(SECTIONS):
        saved_inputs.append(hidden)
        normed, preact, hidden = section_forward(hidden, masked_list[section_index], norm_gain[section_index])
        saved_normed.append(normed)
        saved_preact.append(preact)
    gradients = [None] * SECTIONS
    for section_index in reversed(range(SECTIONS)):
        grad_pre, upstream = section_backward(saved_inputs[section_index], saved_preact[section_index], upstream, masked_list[section_index], norm_gain[section_index])
        dense_part = replica_terms(saved_normed[section_index], grad_pre, micro_count) / math.sqrt(TOKENS)
        decay_part = jnp.where(kept_list[section_index], 0.0, weight[section_index].astype(jnp.float32))
        gradients[section_index] = dense_part + decay_rate * decay_part
    flip_list = []
    for section_index in range(SECTIONS):
        earlier_kept = kept_positions(earlier_mask[section_index])
        flip_list.append(jnp.sum(kept_list[section_index] != earlier_kept).astype(jnp.int32))
    return (jnp.stack(gradients), jnp.stack(flip_list))
```

```python
import functools
import math

import jax
import jax.numpy as jnp
from jax import lax
from jax.experimental import pallas as pl
from jax.experimental.pallas import tpu as pltpu
from jax.sharding import PartitionSpec as P

MESH = pl.DeviceIdType.MESH
epsilon = 1e-06
decay_rate = 4.0
half_root = 0.7071067811865476
density_scale = 0.3989422804014327
first_table = (0, 0, 0, 1, 1, 2)
second_table = (1, 2, 3, 2, 3, 3)
BF = jnp.bfloat16
F32 = jnp.float32


def pair_ends(indices):
    leading = jnp.zeros_like(indices)
    trailing = jnp.zeros_like(indices)
    for pair_index in range(6):
        matches = indices == pair_index
        leading = jnp.where(matches, first_table[pair_index], leading)
        trailing = jnp.where(matches, second_table[pair_index], trailing)
    return (leading, trailing)


def kept_positions(indices):
    leading, trailing = pair_ends(indices)
    groups, columns = indices.shape
    positions = lax.broadcasted_iota(jnp.int32, (groups, 4, columns), 1)
    kept_mask = (positions == leading[:, None, :]) | (positions == trailing[:, None, :])
    return kept_mask.reshape(groups * 4, columns)


def pipeline_kernel(micros, sections, x_hbm, ct_hbm, w_hbm, gain_ref, out_ref, w, hin, gin, hout, gout,
                    preact, slope, normed, grad_pre, scale, w_sem, x_sem, f_send, f_recv, b_send, b_recv):
    s = lax.axis_index("section")
    last = sections - 1
    rows_all, width = hin.shape
    rows = rows_all // micros
    chunk = min(512, width)
    chunks = width // chunk

    first_stage, last_stage = s == 0, s == last
    w_copies = [
        pltpu.make_async_copy(w_hbm.at[pl.ds(k * chunk, chunk)], w.at[pl.ds(k * chunk, chunk)], w_sem.at[k])
        for k in range(chunks)
    ]
    for copy in w_copies:
        copy.start()
    x_copy = pltpu.make_async_copy(x_hbm, hin, x_sem.at[0])
    ct_copy = pltpu.make_async_copy(ct_hbm, gin, x_sem.at[1])

    @pl.when(first_stage)
    def _():
        x_copy.start()

    @pl.when(last_stage)
    def _():
        ct_copy.start()

    barrier = pltpu.get_barrier_semaphore()

    @pl.when(s > 0)
    def _():
        pl.semaphore_signal(barrier, inc=1, device_id={"section": s - 1}, device_id_type=MESH)

    @pl.when(s < last)
    def _():
        pl.semaphore_signal(barrier, inc=1, device_id={"section": s + 1}, device_id_type=MESH)

    pl.semaphore_wait(barrier, jnp.where(s > 0, 1, 0) + jnp.where(s < last, 1, 0))

    for copy in w_copies:
        copy.wait()

    @pl.when(first_stage)
    def _():
        x_copy.wait()

    @pl.when(last_stage)
    def _():
        ct_copy.wait()

    def forward_copy(m, where):
        return pltpu.make_async_remote_copy(
            src_ref=hout.at[where], dst_ref=hin.at[where], send_sem=f_send.at[m], recv_sem=f_recv.at[m],
            device_id={"section": jnp.minimum(s + 1, last)}, device_id_type=MESH)

    def backward_copy(m, where):
        return pltpu.make_async_remote_copy(
            src_ref=gout.at[where], dst_ref=gin.at[where], send_sem=b_send.at[m], recv_sem=b_recv.at[m],
            device_id={"section": jnp.maximum(s - 1, 0)}, device_id_type=MESH)

    gain = gain_ref[...]

    def forward(m, carry):
        at = pl.ds(pl.multiple_of(m * rows, rows), rows)

        @pl.when(s > 0)
        def _():
            forward_copy(m, (at,)).wait_recv()

        values = hin[at, :].astype(F32)
        q = lax.rsqrt(jnp.sum(values * values, axis=-1, keepdims=True) * (1.0 / width) + epsilon)
        scale[at, :] = jnp.broadcast_to(q, (rows, 128))
        normal = (values * q * gain).astype(BF)
        normed[at, :] = normal
        for c in range(chunks):
            cols = pl.ds(c * chunk, chunk)
            p = jnp.dot(normal, w[:, cols], preferred_element_type=F32)
            cdf = 0.5 * (1.0 + lax.erf(p * half_root))
            hout[at, cols] = (hin[at, cols].astype(F32) + p * cdf).astype(BF)

            @pl.when(s < last)
            def _():
                forward_copy(m, (at, cols)).start()

            preact[at, cols] = p
            slope[at, cols] = cdf + p * (jnp.exp(-0.5 * p * p) * density_scale)
        return carry

    lax.fori_loop(0, micros, forward, 0)

    def backward(m, carry):
        at = pl.ds(pl.multiple_of(m * rows, rows), rows)

        @pl.when(s < last)
        def _():
            backward_copy(m, (at,)).wait_recv()

        gp = (gin[at, :].astype(F32) * slope[at, :]).astype(BF)
        grad_pre[at, :] = gp
        q = scale[at, 0:1]
        mean = jnp.sum(gp.astype(F32) * preact[at, :], axis=-1, keepdims=True) * (1.0 / width)
        pull = q * q * mean

        @pl.when(s > 0)
        def _():
            for c in range(chunks):
                cols = pl.ds(c * chunk, chunk)
                a = lax.dot_general(gp, w[cols, :], (((1,), (1,)), ((), ())), preferred_element_type=F32)
                a = a * gain_ref[:, cols]
                gout[at, cols] = (gin[at, cols].astype(F32) + q * a - hin[at, cols].astype(F32) * pull).astype(BF)
                backward_copy(m, (at, cols)).start()
        return carry

    lax.fori_loop(0, micros, backward, 0)

    tile = 256 if width % 256 == 0 else 128

    def terms(i, carry):
        cols = pl.ds(pl.multiple_of(i * tile, tile), tile)
        out_ref[cols, :] = lax.dot_general(
            normed[:, cols], grad_pre[...], (((0,), (0,)), ((), ())), preferred_element_type=F32).astype(BF)
        return carry

    lax.fori_loop(0, width // tile, terms, 0)

    def drain(m, carry):
        at = pl.ds(pl.multiple_of(m * rows, rows), rows)

        @pl.when(s < last)
        def _():
            forward_copy(m, (at,)).wait_send()

        @pl.when(s > 0)
        def _():
            backward_copy(m, (at,)).wait_send()

        return carry

    lax.fori_loop(0, micros, drain, 0)


def pipeline(x, ct, masked, gain, sections, micros):
    rows, width = x.shape
    chunks = width // min(512, width)
    vmem = pl.BlockSpec(memory_space=pltpu.VMEM)
    hbm = pl.BlockSpec(memory_space=pl.ANY)
    act = pltpu.VMEM((rows, width), BF)
    wide = pltpu.VMEM((rows, width), F32)
    dma = pltpu.SemaphoreType.DMA
    return pl.pallas_call(
        functools.partial(pipeline_kernel, micros, sections),
        out_shape=jax.ShapeDtypeStruct((width, width), BF),
        in_specs=[hbm, hbm, hbm, vmem],
        out_specs=vmem,
        scratch_shapes=[
            pltpu.VMEM((width, width), BF), act, act, act, act, wide, wide, act, act, pltpu.VMEM((rows, 128), F32),
            dma((chunks,)), dma((2,)), dma((micros,)), dma((micros,)), dma((micros,)), dma((micros,)),
        ],
        compiler_params=pltpu.CompilerParams(
            collective_id=0, has_side_effects=True, vmem_limit_bytes=48 * 1024 * 1024),
        cost_estimate=pl.CostEstimate(
            flops=6 * rows * width * width, bytes_accessed=4 * width * width, transcendentals=0),
    )(x, ct, masked, gain)


def body(activations, cotangent, weight, norm_gain, pair_mask, earlier_mask):
    section_count = lax.axis_size("section")
    replica_count = lax.axis_size("dp")
    replica_index = lax.axis_index("dp")
    micro_count, row_count, model_width = activations.shape
    shard_rows = weight.shape[1]
    groups = shard_rows // 4
    own_weight = weight[0]
    own_pairs = lax.dynamic_slice_in_dim(pair_mask[0], replica_index * groups, groups, 0)
    own_kept = kept_positions(own_pairs)
    earlier_kept = kept_positions(earlier_mask[0])
    flip_local = jnp.sum(own_kept != earlier_kept).reshape(1)
    flip_sum = lax.psum(flip_local, "dp")
    masked_shard = jnp.where(own_kept, own_weight, jnp.zeros_like(own_weight))
    masked = lax.all_gather(masked_shard, "dp", axis=0, tiled=True)
    tokens = micro_count * row_count
    partial = pipeline(
        activations.reshape(tokens, model_width), cotangent.reshape(tokens, model_width), masked, norm_gain,
        section_count, 8)
    summed = lax.psum_scatter(partial, "dp", scatter_dimension=0, tiled=True).astype(jnp.float32)
    dense_part = summed / math.sqrt(tokens * replica_count)
    decay_part = jnp.where(own_kept, 0.0, own_weight.astype(jnp.float32))
    gradient = dense_part + decay_rate * decay_part
    return (gradient[None], flip_sum)


def solution(mesh):
    placed = (
        P(None, "dp", None),
        P(None, "dp", None),
        P("section", "dp", None),
        P("section", None),
        P("section", None, None),
        P("section", "dp", None),
    )
    return jax.shard_map(
        body,
        mesh=mesh,
        in_specs=placed,
        out_specs=(P("section", "dp", None), P("section")),
        check_vma=False,
    )
```

```python
import functools
import math

import jax
import jax.numpy as jnp
from jax import lax
from jax.experimental import pallas as pl
from jax.experimental.pallas import tpu as pltpu
from jax.sharding import PartitionSpec as P

MESH = pl.DeviceIdType.MESH
epsilon = 1e-06
decay_rate = 4.0
half_root = 0.7071067811865476
density_scale = 0.3989422804014327
BF = jnp.bfloat16
F32 = jnp.float32
SIDE = 4
BLOCKS = SIDE * SIDE


def kernel(micros, sections, token_total, x_hbm, ct_hbm, weight_ref, gain_ref, pair_hbm, earlier_ref, out_ref, flip_ref,
           w, packed, pair, wide_rows, decay, hin, gin, hout, gout, preact, slope, scale, mine, theirs, grad_pre,
           part, part_a, part_b, row_sum, row_a, row_b, flips,
           local_sem, ag_send, ag_recv, mate_recv, f_send, f_recv, b_send, b_recv, mate_n, mate_g, mate_send,
           a_recv, ab_recv, ra_recv, rb_recv, rs_send, flip_send, flip_recv):
    s = lax.axis_index("section")
    dp = lax.axis_index("dp")
    core, xx, yy = dp % 2, (dp // 2) % SIDE, dp // (2 * SIDE)
    last = sections - 1
    rows_all, width = hin.shape
    rows = rows_all // micros
    chunk = 512
    chunks = width // chunk
    shard = weight_ref.shape[0]
    groups = shard // 4
    half_width = width // 2

    def chip(plane, r1, r2):
        dx, dy = jnp.where(plane == 0, r1, r2), jnp.where(plane == 0, r2, r1)
        return ((yy + dy) % SIDE) * SIDE + (xx + dx) % SIDE

    mate = 2 * (dp // 2) + (1 - core)
    right1, left1 = 2 * chip(core, 1, 0) + core, 2 * chip(core, 3, 0) + core
    right2, left2 = 2 * chip(core, 0, 1) + core, 2 * chip(core, 0, 3) + core
    around = (right1, left1, right2, left2)

    def remote(src, dst, send, recv, target):
        return pltpu.make_async_remote_copy(
            src_ref=src, dst_ref=dst, send_sem=send, recv_sem=recv, device_id={"dp": target}, device_id_type=MESH)

    pair_copy = pltpu.make_async_copy(pair_hbm, pair, local_sem.at[0])
    pair_copy.start()
    x_copy = pltpu.make_async_copy(x_hbm, hin, local_sem.at[1])
    ct_copy = pltpu.make_async_copy(ct_hbm, gin, local_sem.at[2])

    @pl.when(s == 0)
    def _():
        x_copy.start()

    @pl.when(s == last)
    def _():
        ct_copy.start()

    barrier = pltpu.get_barrier_semaphore()
    for target in (*around, mate):
        pl.semaphore_signal(barrier, inc=1, device_id={"dp": target}, device_id_type=MESH)

    @pl.when(s > 0)
    def _():
        pl.semaphore_signal(barrier, inc=1, device_id={"section": s - 1}, device_id_type=MESH)

    @pl.when(s < last)
    def _():
        pl.semaphore_signal(barrier, inc=1, device_id={"section": s + 1}, device_id_type=MESH)

    pair_copy.wait()
    own_groups = pl.ds(pl.multiple_of(dp * groups, groups), groups)
    piece = 128
    counted = jnp.zeros((8, 128), jnp.int32)
    for k in range(width // piece):
        cols = pl.ds(k * piece, piece)
        p = pair[own_groups, cols]
        wide_rows[k] = weight_ref[:, cols].astype(F32)
        w0, w1, w2, w3 = (wide_rows[k, pl.ds(j, groups, stride=4), :] for j in range(4))
        lead = jnp.where(p < 3, w0, jnp.where(p == 5, w2, w1))
        trail = jnp.where(p == 0, w1, jnp.where((p == 1) | (p == 3), w2, w3))
        packed[dp, 0:groups, cols] = lead.astype(BF)
        packed[dp, groups:2 * groups, cols] = trail.astype(BF)
        kept = (p < 3, (p == 0) | (p == 3) | (p == 4), (p == 1) | (p == 3) | (p == 5), (p == 2) | (p > 3))
        for j, (k_j, w_j) in enumerate(zip(kept, (w0, w1, w2, w3))):
            decay[k, pl.ds(j, groups, stride=4), :] = jnp.where(k_j, 0.0, decay_rate * w_j)
        e = earlier_ref[:, cols]
        changed = jnp.where(p == e, 0, jnp.where(p + e == 5, 4, 2))
        for a in range(groups // 8):
            for b in range(piece // 128):
                counted = counted + changed[8 * a:8 * a + 8, 128 * b:128 * b + 128]
    flips[0] = counted

    pl.semaphore_wait(barrier, 5 + jnp.where(s > 0, 1, 0) + jnp.where(s < last, 1, 0))

    def send_half(b, h, d):
        at = pl.ds(h * groups, groups)
        remote(packed.at[2 * b + core, at], packed.at[2 * b + core, at], ag_send.at[d], ag_recv.at[b, h],
               around[d]).start()

    def send_mate(b):
        remote(packed.at[2 * b + core], packed.at[2 * b + core], ag_send.at[4], mate_recv.at[b], mate).start()

    def wait_half(b, h):
        at = pl.ds(h * groups, groups)
        remote(packed.at[2 * b + core, at], packed.at[2 * b + core, at], ag_send.at[0], ag_recv.at[b, h],
               mate).wait_recv()

    def wait_mate(b):
        slot = 2 * b + (1 - core)
        remote(packed.at[slot], packed.at[slot], ag_send.at[4], mate_recv.at[b], mate).wait_recv()

    def spread(b):
        for d in (2, 3):
            send_half(b, 0, d)
            send_half(b, 1, d)
        send_mate(b)

    def unpack(slot):
        at = pl.ds(pl.multiple_of(slot * groups, groups), groups)
        to = pl.ds(pl.multiple_of(slot * shard, shard), shard)
        for k in range(width // piece):
            cols = pl.ds(k * piece, piece)
            p = pair[at, cols]
            lead = packed[slot, 0:groups, cols].astype(F32)
            trail = packed[slot, groups:2 * groups, cols].astype(F32)
            o0 = jnp.where(p < 3, lead, 0.0)
            o1 = jnp.where(p == 0, trail, jnp.where((p == 3) | (p == 4), lead, 0.0))
            o2 = jnp.where(p == 5, lead, jnp.where((p == 1) | (p == 3), trail, 0.0))
            o3 = jnp.where((p == 2) | (p > 3), trail, 0.0)
            for j, o in enumerate((o0, o1, o2, o3)):
                wide_rows[k, pl.ds(j, groups, stride=4), :] = o
            w[to, cols] = wide_rows[k].astype(BF)

    def flip_copy(src, dst, target):
        return remote(flips.at[src], flips.at[dst], flip_send.at[dst - 1], flip_recv.at[dst - 1], target)

    own = chip(core, 0, 0)
    for d in (0, 1):
        send_half(own, 0, d)
        send_half(own, 1, d)
    spread(own)
    flip_copy(0, 1, mate).start()
    unpack(dp)
    from_left, from_right, far = chip(core, 3, 0), chip(core, 1, 0), chip(core, 2, 0)
    wait_half(from_left, 0)
    send_half(from_left, 0, 0)
    wait_half(from_left, 1)
    spread(from_left)
    wait_half(from_right, 1)
    send_half(from_right, 1, 1)
    wait_half(from_right, 0)
    spread(from_right)
    flip_copy(0, 1, mate).wait_recv()
    flips[8] = flips[0] + flips[1]
    flip_copy(8, 2, right1).start()
    flip_copy(8, 3, left1).start()
    unpack(2 * from_left + core)
    wait_half(far, 0)
    wait_half(far, 1)
    spread(far)

    def near(i, carry):
        r1 = jnp.where(i == 0, 0, jnp.where(i == 1, 3, jnp.where(i == 2, 1, 2)))
        lower, upper = chip(core, r1, 3), chip(core, r1, 1)
        wait_half(lower, 0)
        send_half(lower, 0, 2)
        wait_half(lower, 1)
        send_mate(lower)
        wait_half(upper, 1)
        send_half(upper, 1, 3)
        wait_half(upper, 0)
        send_mate(upper)
        other = chip(1 - core, r1, 0)
        wait_mate(other)

        def expand(j, c):
            unpack(jnp.where(j == 0, 2 * other + (1 - core), jnp.where(j == 1, 2 * lower + core, 2 * upper + core)))
            return c

        lax.fori_loop(0, 3, expand, 0)
        return carry

    lax.fori_loop(0, SIDE, near, 0)

    def expand_rest(j, c):
        unpack(2 * jnp.where(j == 0, from_right, far) + core)
        return c

    lax.fori_loop(0, 2, expand_rest, 0)
    flip_copy(8, 2, right1).wait_recv()
    flip_copy(2, 4, right1).start()

    def distant(i, carry):
        r1 = jnp.where(i == 0, 0, jnp.where(i == 1, 3, jnp.where(i == 2, 1, 2)))
        beyond = chip(core, r1, 2)
        wait_half(beyond, 0)
        wait_half(beyond, 1)
        send_mate(beyond)
        lower, upper = chip(1 - core, r1, 3), chip(1 - core, r1, 1)
        wait_mate(lower)
        wait_mate(upper)

        def expand(j, c):
            unpack(jnp.where(j == 0, 2 * beyond + core,
                             jnp.where(j == 1, 2 * lower + (1 - core), 2 * upper + (1 - core))))
            return c

        lax.fori_loop(0, 3, expand, 0)
        return carry

    lax.fori_loop(0, SIDE, distant, 0)

    def final(i, carry):
        r1 = jnp.where(i == 0, 0, jnp.where(i == 1, 3, jnp.where(i == 2, 1, 2)))
        b = chip(1 - core, r1, 2)
        wait_mate(b)
        unpack(2 * b + (1 - core))
        return carry

    lax.fori_loop(0, SIDE, final, 0)

    flip_copy(8, 3, left1).wait_recv()
    flip_copy(2, 4, right1).wait_recv()
    flips[9] = flips[8] + flips[2] + flips[3] + flips[4]
    flip_copy(9, 5, right2).start()
    flip_copy(9, 6, left2).start()

    @pl.when(s == 0)
    def _():
        x_copy.wait()

    @pl.when(s == last)
    def _():
        ct_copy.wait()

    def z_copy(src, dst, send, recv, where, target):
        return pltpu.make_async_remote_copy(
            src_ref=src.at[where], dst_ref=dst.at[where], send_sem=send, recv_sem=recv,
            device_id={"section": target}, device_id_type=MESH)

    def forward_copy(m, where):
        return z_copy(hout, hin, f_send.at[m], f_recv.at[m], where, jnp.minimum(s + 1, last))

    def backward_copy(m, where):
        return z_copy(gout, gin, b_send.at[m], b_recv.at[m], where, jnp.maximum(s - 1, 0))

    def mate_copy(src, dst, sems, k, m):
        at = pl.ds(pl.multiple_of(m * rows, rows), rows)
        to = pl.ds(pl.multiple_of(rows_all + m * rows, rows), rows)
        return remote(src.at[at], dst.at[to], mate_send.at[k, m], sems.at[m], mate)

    def forward(m, carry):
        at = pl.ds(pl.multiple_of(m * rows, rows), rows)

        @pl.when(s > 0)
        def _():
            forward_copy(m, (at,)).wait_recv()

        values = hin[at, :].astype(F32)
        q = lax.rsqrt(jnp.sum(values * values, axis=-1, keepdims=True) * (1.0 / width) + epsilon)
        scale[at, :] = jnp.broadcast_to(q, (rows, 128))
        normal = (values * q * gain_ref[...]).astype(BF)
        for c in range(chunks):
            cols = pl.ds(c * chunk, chunk)
            p = jnp.dot(normal, w[:, cols], preferred_element_type=F32)
            cdf = 0.5 * (1.0 + lax.erf(p * half_root))
            hout[at, cols] = (hin[at, cols].astype(F32) + p * cdf).astype(BF)

            @pl.when(s < last)
            def _():
                forward_copy(m, (at, cols)).start()

            preact[at, cols] = p
            slope[at, cols] = cdf + p * (jnp.exp(-0.5 * p * p) * density_scale)
        low = lax.broadcasted_iota(jnp.int32, (rows, 128), 1) < 64
        for k in range(width // 256):
            first = hin[at, pl.ds(256 * k, 128)].astype(F32) * q * gain_ref[:, pl.ds(256 * k, 128)]
            second = hin[at, pl.ds(256 * k + 128, 128)].astype(F32) * q * gain_ref[:, pl.ds(256 * k + 128, 128)]
            even = jnp.where(low, first, pltpu.roll(second, 64, 1))
            odd = jnp.where(low, pltpu.roll(first, 64, 1), second)
            cols = pl.ds(128 * k, 128)
            mine[at, cols] = jnp.where(core == 0, even, odd).astype(BF)
            theirs[at, cols] = jnp.where(core == 0, odd, even).astype(BF)
        mate_copy(theirs, mine, mate_n, 0, m).start()
        return carry

    lax.fori_loop(0, micros, forward, 0)

    flip_copy(9, 5, right2).wait_recv()
    flip_copy(5, 7, right2).start()

    def backward(m, carry):
        at = pl.ds(pl.multiple_of(m * rows, rows), rows)

        @pl.when(s < last)
        def _():
            backward_copy(m, (at,)).wait_recv()

        gp = (gin[at, :].astype(F32) * slope[at, :]).astype(BF)
        grad_pre[at, :] = gp
        mate_copy(grad_pre, grad_pre, mate_g, 1, m).start()

        @pl.when(s > 0)
        def _():
            q = scale[at, 0:1]
            mean = jnp.sum(gp.astype(F32) * preact[at, :], axis=-1, keepdims=True) * (1.0 / width)
            pull = q * q * mean
            for c in range(chunks):
                cols = pl.ds(c * chunk, chunk)
                a = lax.dot_general(gp, w[cols, :], (((1,), (1,)), ((), ())), preferred_element_type=F32)
                a = a * gain_ref[:, cols]
                gout[at, cols] = (gin[at, cols].astype(F32) + q * a - hin[at, cols].astype(F32) * pull).astype(BF)
                backward_copy(m, (at, cols)).start()
        return carry

    lax.fori_loop(0, micros, backward, 0)

    def mate_rows(m, carry):
        mate_copy(theirs, mine, mate_n, 0, m).wait_recv()
        mate_copy(grad_pre, grad_pre, mate_g, 1, m).wait_recv()
        return carry

    lax.fori_loop(0, micros, mate_rows, 0)

    def terms(i, carry):
        cols = pl.ds(pl.multiple_of(i * 256, 256), 256)
        part[cols, :] = lax.dot_general(
            mine[:, cols], grad_pre[...], (((0,), (0,)), ((), ())), preferred_element_type=F32).astype(BF)
        return carry

    lax.fori_loop(0, half_width // 256, terms, 0)

    def block(r1, r2):
        return pl.ds(pl.multiple_of(chip(core, r1, r2) * shard, shard), shard)

    def slot(r2, count=1):
        return pl.ds(r2 * shard, count * shard)

    def first_ring(src_r1, r2, d, dst, dst_slot, recv):
        return remote(part.at[block(src_r1, r2)], dst.at[dst_slot], rs_send.at[d], recv, around[d])

    toward_left, toward_right = (2, 1), (3, 0)
    for r2 in toward_left:
        first_ring(2, r2, 1, part_a, slot(r2), a_recv.at[r2]).start()
    for r2 in toward_right:
        first_ring(2, r2, 0, part_a, slot(r2), a_recv.at[r2]).start()
    for r2 in toward_right:
        first_ring(3, r2, 1, part_b, slot(r2), ab_recv.at[0, r2]).start()
    for r2 in toward_left:
        first_ring(1, r2, 0, part_b, slot(4 + r2), ab_recv.at[1, r2]).start()
    for k in range(2):
        for r2, r1, d, side in ((toward_left[k], 3, 1, 0), (toward_right[k], 1, 0, 1)):
            first_ring(2, r2, d, part_a, slot(r2), a_recv.at[r2]).wait_recv()
            at = block(r1, r2)
            part[at, :] = (part[at, :].astype(F32) + part_a[slot(r2), :].astype(F32)).astype(BF)
            first_ring(r1, r2, d, part_b, slot(4 * side + r2), ab_recv.at[side, r2]).start()

    flip_copy(9, 6, left2).wait_recv()
    flip_copy(5, 7, right2).wait_recv()
    all_flips = flips[9] + flips[5] + flips[6] + flips[7]
    flip_ref[0] = jnp.sum(all_flips.astype(F32)).astype(jnp.int32)

    def ring_total(r2):
        for side in range(2):
            first_ring(3, r2, 1, part_b, slot(4 * side + r2), ab_recv.at[side, r2]).wait_recv()
        total = part[block(0, r2), :].astype(F32) + part_b[slot(r2), :].astype(F32) + part_b[slot(4 + r2), :].astype(F32)
        row_sum[slot(r2), :] = total.astype(BF)

    half = shard // 2

    def second_ring(r2, h, d, dst, start, recv):
        return remote(row_sum.at[pl.ds(r2 * shard + h * half, half)], dst.at[pl.ds(start, half)], rs_send.at[d], recv,
                      around[d])

    ring_total(2)
    second_ring(2, 0, 3, row_a, 0, ra_recv.at[0]).start()
    second_ring(2, 1, 2, row_a, half, ra_recv.at[1]).start()
    ring_total(3)
    second_ring(3, 1, 3, row_b, half, rb_recv.at[0, 1]).start()
    ring_total(1)
    second_ring(1, 0, 2, row_b, shard, rb_recv.at[1, 0]).start()
    for h, r2, d, side in ((0, 3, 3, 0), (1, 1, 2, 1)):
        second_ring(2, h, d, row_a, h * half, ra_recv.at[h]).wait_recv()
        at = pl.ds(r2 * shard + h * half, half)
        row_sum[at, :] = (row_sum[at, :].astype(F32) + row_a[pl.ds(h * half, half), :].astype(F32)).astype(BF)
        second_ring(r2, h, d, row_b, side * shard + h * half, rb_recv.at[side, h]).start()
    ring_total(0)
    for side, h in ((0, 1), (1, 0), (0, 0), (1, 1)):
        second_ring(2, h, 3, row_b, side * shard + h * half, rb_recv.at[side, h]).wait_recv()
    for k in range(width // piece):
        cols = pl.ds(k * piece, piece)
        total = row_sum[slot(0), cols].astype(F32) + row_b[slot(0), cols].astype(F32) + row_b[slot(1), cols].astype(F32)
        out_ref[:, cols] = total * (1.0 / math.sqrt(token_total)) + decay[k]

    def drain(m, carry):
        at = pl.ds(pl.multiple_of(m * rows, rows), rows)

        @pl.when(s < last)
        def _():
            forward_copy(m, (at,)).wait_send()

        @pl.when(s > 0)
        def _():
            backward_copy(m, (at,)).wait_send()

        mate_copy(theirs, mine, mate_n, 0, m).wait_send()
        mate_copy(grad_pre, grad_pre, mate_g, 1, m).wait_send()
        return carry

    lax.fori_loop(0, micros, drain, 0)

    def sent(sem, count):
        ref = grad_pre.at[pl.ds(0, count)]
        remote(ref, ref, sem, flip_recv.at[0], mate).wait_send()

    for d in (0, 1):
        sent(ag_send.at[d], 3 * groups)
    for d in (2, 3):
        sent(ag_send.at[d], 12 * groups)
    sent(ag_send.at[4], 2 * BLOCKS * groups)
    for d in (0, 1):
        sent(rs_send.at[d], 6 * shard)
    for d in (2, 3):
        sent(rs_send.at[d], 3 * half)
    for dst in range(1, 8):
        flip_copy(0, dst, mate).wait_send()


def step(x, ct, weight, gain, pair, earlier, sections, token_total, micros):
    rows, width = x.shape
    shard = weight.shape[0]
    groups = shard // 4
    vmem = pl.BlockSpec(memory_space=pltpu.VMEM)
    hbm = pl.BlockSpec(memory_space=pl.ANY)
    act = pltpu.VMEM((rows, width), BF)
    wide = pltpu.VMEM((rows, width), F32)
    dma = pltpu.SemaphoreType.DMA
    return pl.pallas_call(
        functools.partial(kernel, micros, sections, token_total),
        out_shape=(jax.ShapeDtypeStruct((shard, width), F32), jax.ShapeDtypeStruct((1,), jnp.int32)),
        in_specs=[hbm, hbm, vmem, vmem, hbm, vmem],
        out_specs=(vmem, pl.BlockSpec(memory_space=pltpu.SMEM)),
        scratch_shapes=[
            pltpu.VMEM((width, width), BF),
            pltpu.VMEM((2 * BLOCKS, 2 * groups, width), BF),
            pltpu.VMEM(pair.shape, jnp.int32),
            pltpu.VMEM((width // 128, shard, 128), F32),
            pltpu.VMEM((width // 128, shard, 128), F32),
            act, act, act, act, wide, wide, pltpu.VMEM((rows, 128), F32),
            pltpu.VMEM((2 * rows, width // 2), BF),
            pltpu.VMEM((rows, width // 2), BF),
            pltpu.VMEM((2 * rows, width), BF),
            pltpu.VMEM((width // 2, width), BF),
            pltpu.VMEM((SIDE * shard, width), BF),
            pltpu.VMEM((2 * SIDE * shard, width), BF),
            pltpu.VMEM((SIDE * shard, width), BF),
            pltpu.VMEM((shard, width), BF),
            pltpu.VMEM((2 * shard, width), BF),
            pltpu.VMEM((10, 8, 128), jnp.int32),
            dma((3,)), dma((5,)), dma((BLOCKS, 2)), dma((BLOCKS,)),
            dma((micros,)), dma((micros,)), dma((micros,)), dma((micros,)),
            dma((micros,)), dma((micros,)), dma((2, micros)),
            dma((SIDE,)), dma((2, SIDE)), dma((2,)), dma((2, 2)), dma((4,)), dma((7,)), dma((7,)),
        ],
        compiler_params=pltpu.CompilerParams(
            collective_id=0, has_side_effects=True, vmem_limit_bytes=56 * 1024 * 1024),
    )(x, ct, weight, gain, pair, earlier)


def body(activations, cotangent, weight, norm_gain, pair_mask, earlier_mask):
    micro_count, row_count, model_width = activations.shape
    tokens = micro_count * row_count
    gradient, flip_sum = step(
        activations.reshape(tokens, model_width), cotangent.reshape(tokens, model_width), weight[0], norm_gain,
        pair_mask[0], earlier_mask[0], lax.axis_size("section"), tokens * lax.axis_size("dp"), 8)
    return (gradient[None], flip_sum)


def solution(mesh):
    placed = (
        P(None, "dp", None),
        P(None, "dp", None),
        P("section", "dp", None),
        P("section", None),
        P("section", None, None),
        P("section", "dp", None),
    )
    return jax.shard_map(
        body,
        mesh=mesh,
        in_specs=placed,
        out_specs=(P("section", "dp", None), P("section")),
        check_vma=False,
    )
```

```python
import functools
import math

import jax
import jax.numpy as jnp
from jax import lax
from jax.experimental import pallas as pl
from jax.experimental.pallas import tpu as pltpu
from jax.sharding import PartitionSpec as P

MESH = pl.DeviceIdType.MESH
epsilon = 1e-06
decay_rate = 4.0
half_root = 0.7071067811865476
density_scale = 0.3989422804014327
BF = jnp.bfloat16
F32 = jnp.float32
SIDE = 4
BLOCKS = SIDE * SIDE


def kernel(micros, sections, token_total, x_hbm, ct_hbm, weight_ref, gain_ref, pair_hbm, earlier_ref, out_ref, flip_ref,
           w, turned, packed, pair, wide_rows, decay, arriving, leaving, hidden, preact, slope, scale, mine, theirs,
           grad_pre, part, part_a, part_b, row_sum, row_a, row_b, flips,
           local_sem, ag_send, ag_recv, mate_recv, in_send, in_recv, z_send, z_recv, mate_n, mate_g, mate_f, mate_send,
           a_recv, ab_recv, ra_recv, rb_recv, rs_send, flip_send, flip_recv):
    s = lax.axis_index("section")
    dp = lax.axis_index("dp")
    core, xx, yy = dp % 2, (dp // 2) % SIDE, dp // (2 * SIDE)
    last = sections - 1
    rows_all, width = arriving.shape
    rows = rows_all // micros
    half_rows = rows_all // 2
    forward_core, backward_core = core == 1, core == 0
    chunk = 512
    chunks = width // chunk
    shard = weight_ref.shape[0]
    groups = shard // 4
    half_width = width // 2

    def chip(plane, r1, r2):
        dx, dy = jnp.where(plane == 0, r1, r2), jnp.where(plane == 0, r2, r1)
        return ((yy + dy) % SIDE) * SIDE + (xx + dx) % SIDE

    mate = 2 * (dp // 2) + (1 - core)
    right1, left1 = 2 * chip(core, 1, 0) + core, 2 * chip(core, 3, 0) + core
    right2, left2 = 2 * chip(core, 0, 1) + core, 2 * chip(core, 0, 3) + core
    around = (right1, left1, right2, left2)

    def remote(src, dst, send, recv, target):
        return pltpu.make_async_remote_copy(
            src_ref=src, dst_ref=dst, send_sem=send, recv_sem=recv, device_id={"dp": target}, device_id_type=MESH)

    pair_copy = pltpu.make_async_copy(pair_hbm, pair, local_sem.at[0])
    pair_copy.start()
    x_copy = pltpu.make_async_copy(x_hbm, arriving.at[pl.ds(0, half_rows)], local_sem.at[1])
    ct_copy = pltpu.make_async_copy(ct_hbm, arriving.at[pl.ds(half_rows, half_rows)], local_sem.at[1])
    x_mate = remote(x_hbm, arriving.at[pl.ds(half_rows, half_rows)], in_send.at[0], in_recv.at[0], mate)
    ct_mate = remote(ct_hbm, arriving.at[pl.ds(0, half_rows)], in_send.at[0], in_recv.at[0], mate)

    @pl.when((s == 0) & forward_core)
    def _():
        x_copy.start()

    @pl.when((s == last) & backward_core)
    def _():
        ct_copy.start()

    barrier = pltpu.get_barrier_semaphore()
    for target in (*around, mate):
        pl.semaphore_signal(barrier, inc=1, device_id={"dp": target}, device_id_type=MESH)

    @pl.when(s > 0)
    def _():
        pl.semaphore_signal(barrier, inc=1, device_id={"section": s - 1}, device_id_type=MESH)

    @pl.when(s < last)
    def _():
        pl.semaphore_signal(barrier, inc=1, device_id={"section": s + 1}, device_id_type=MESH)

    pair_copy.wait()
    own_groups = pl.ds(pl.multiple_of(dp * groups, groups), groups)
    piece = 128
    counted = jnp.zeros((8, 128), jnp.int32)
    for k in range(width // piece):
        cols = pl.ds(k * piece, piece)
        p = pair[own_groups, cols]
        wide_rows[k] = weight_ref[:, cols].astype(F32)
        w0, w1, w2, w3 = (wide_rows[k, pl.ds(j, groups, stride=4), :] for j in range(4))
        lead = jnp.where(p < 3, w0, jnp.where(p == 5, w2, w1))
        trail = jnp.where(p == 0, w1, jnp.where((p == 1) | (p == 3), w2, w3))
        packed[dp, 0:groups, cols] = lead.astype(BF)
        packed[dp, groups:2 * groups, cols] = trail.astype(BF)
        kept = (p < 3, (p == 0) | (p == 3) | (p == 4), (p == 1) | (p == 3) | (p == 5), (p == 2) | (p > 3))
        for j, (k_j, w_j) in enumerate(zip(kept, (w0, w1, w2, w3))):
            decay[k, pl.ds(j, groups, stride=4), :] = jnp.where(k_j, 0.0, decay_rate * w_j)
        e = earlier_ref[:, cols]
        changed = jnp.where(p == e, 0, jnp.where(p + e == 5, 4, 2))
        for a in range(groups // 8):
            for b in range(piece // 128):
                counted = counted + changed[8 * a:8 * a + 8, 128 * b:128 * b + 128]
    flips[0] = counted

    pl.semaphore_wait(barrier, 5 + jnp.where(s > 0, 1, 0) + jnp.where(s < last, 1, 0))

    @pl.when((s == 0) & backward_core)
    def _():
        x_mate.start()

    @pl.when((s == last) & forward_core)
    def _():
        ct_mate.start()

    def send_half(b, h, d):
        at = pl.ds(h * groups, groups)
        remote(packed.at[2 * b + core, at], packed.at[2 * b + core, at], ag_send.at[d], ag_recv.at[b, h],
               around[d]).start()

    def send_mate(b):
        remote(packed.at[2 * b + core], packed.at[2 * b + core], ag_send.at[4], mate_recv.at[b], mate).start()

    def wait_half(b, h):
        at = pl.ds(h * groups, groups)
        remote(packed.at[2 * b + core, at], packed.at[2 * b + core, at], ag_send.at[0], ag_recv.at[b, h],
               mate).wait_recv()

    def wait_mate(b):
        slot = 2 * b + (1 - core)
        remote(packed.at[slot], packed.at[slot], ag_send.at[4], mate_recv.at[b], mate).wait_recv()

    def spread(b):
        for d in (2, 3):
            send_half(b, 0, d)
            send_half(b, 1, d)
        send_mate(b)

    def unpack(slot):
        at = pl.ds(pl.multiple_of(slot * groups, groups), groups)
        to = pl.ds(pl.multiple_of(slot * shard, shard), shard)
        for k in range(width // piece):
            cols = pl.ds(k * piece, piece)
            p = pair[at, cols]
            lead = packed[slot, 0:groups, cols].astype(F32)
            trail = packed[slot, groups:2 * groups, cols].astype(F32)
            o0 = jnp.where(p < 3, lead, 0.0)
            o1 = jnp.where(p == 0, trail, jnp.where((p == 3) | (p == 4), lead, 0.0))
            o2 = jnp.where(p == 5, lead, jnp.where((p == 1) | (p == 3), trail, 0.0))
            o3 = jnp.where((p == 2) | (p > 3), trail, 0.0)
            for j, o in enumerate((o0, o1, o2, o3)):
                wide_rows[k, pl.ds(j, groups, stride=4), :] = o
            w[to, cols] = wide_rows[k].astype(BF)

    def flip_copy(src, dst, target):
        return remote(flips.at[src], flips.at[dst], flip_send.at[dst - 1], flip_recv.at[dst - 1], target)

    own = chip(core, 0, 0)
    for d in (0, 1):
        send_half(own, 0, d)
        send_half(own, 1, d)
    spread(own)
    flip_copy(0, 1, mate).start()
    unpack(dp)
    from_left, from_right, far = chip(core, 3, 0), chip(core, 1, 0), chip(core, 2, 0)
    wait_half(from_left, 0)
    send_half(from_left, 0, 0)
    wait_half(from_left, 1)
    spread(from_left)
    wait_half(from_right, 1)
    send_half(from_right, 1, 1)
    wait_half(from_right, 0)
    spread(from_right)
    flip_copy(0, 1, mate).wait_recv()
    flips[8] = flips[0] + flips[1]
    flip_copy(8, 2, right1).start()
    flip_copy(8, 3, left1).start()
    unpack(2 * from_left + core)
    wait_half(far, 0)
    wait_half(far, 1)
    spread(far)

    def near(i, carry):
        r1 = jnp.where(i == 0, 0, jnp.where(i == 1, 3, jnp.where(i == 2, 1, 2)))
        lower, upper = chip(core, r1, 3), chip(core, r1, 1)
        wait_half(lower, 0)
        send_half(lower, 0, 2)
        wait_half(lower, 1)
        send_mate(lower)
        wait_half(upper, 1)
        send_half(upper, 1, 3)
        wait_half(upper, 0)
        send_mate(upper)
        other = chip(1 - core, r1, 0)
        wait_mate(other)

        def expand(j, c):
            unpack(jnp.where(j == 0, 2 * other + (1 - core), jnp.where(j == 1, 2 * lower + core, 2 * upper + core)))
            return c

        lax.fori_loop(0, 3, expand, 0)
        return carry

    lax.fori_loop(0, SIDE, near, 0)

    def expand_rest(j, c):
        unpack(2 * jnp.where(j == 0, from_right, far) + core)
        return c

    lax.fori_loop(0, 2, expand_rest, 0)
    flip_copy(8, 2, right1).wait_recv()
    flip_copy(2, 4, right1).start()

    def distant(i, carry):
        r1 = jnp.where(i == 0, 0, jnp.where(i == 1, 3, jnp.where(i == 2, 1, 2)))
        beyond = chip(core, r1, 2)
        wait_half(beyond, 0)
        wait_half(beyond, 1)
        send_mate(beyond)
        lower, upper = chip(1 - core, r1, 3), chip(1 - core, r1, 1)
        wait_mate(lower)
        wait_mate(upper)

        def expand(j, c):
            unpack(jnp.where(j == 0, 2 * beyond + core,
                             jnp.where(j == 1, 2 * lower + (1 - core), 2 * upper + (1 - core))))
            return c

        lax.fori_loop(0, 3, expand, 0)
        return carry

    lax.fori_loop(0, SIDE, distant, 0)

    def final(i, carry):
        r1 = jnp.where(i == 0, 0, jnp.where(i == 1, 3, jnp.where(i == 2, 1, 2)))
        b = chip(1 - core, r1, 2)
        wait_mate(b)
        unpack(2 * b + (1 - core))
        return carry

    lax.fori_loop(0, SIDE, final, 0)

    flip_copy(8, 3, left1).wait_recv()
    flip_copy(2, 4, right1).wait_recv()
    flips[9] = flips[8] + flips[2] + flips[3] + flips[4]
    flip_copy(9, 5, right2).start()
    flip_copy(9, 6, left2).start()

    def tile_rows(m):
        return pl.ds(pl.multiple_of(m * rows, rows), rows)

    def z_copy(m, where, target):
        return pltpu.make_async_remote_copy(
            src_ref=leaving.at[where], dst_ref=arriving.at[where], send_sem=z_send.at[m], recv_sem=z_recv.at[m],
            device_id={"section": target}, device_id_type=MESH)

    def forward_copy(m, where):
        return z_copy(m, where, jnp.minimum(s + 1, last))

    def backward_copy(m, where):
        return z_copy(m, where, jnp.maximum(s - 1, 0))

    def half_copy(m):
        return remote(theirs.at[tile_rows(m)], mine.at[tile_rows(m)], mate_send.at[0, m], mate_n.at[m], mate)

    def grad_copy(m):
        return remote(grad_pre.at[tile_rows(m)], grad_pre.at[tile_rows(m)], mate_send.at[0, m], mate_g.at[m], mate)

    def saved_copy(k, m):
        src = (arriving, slope, preact, scale)[k]
        dst = (hidden, slope, preact, scale)[k]
        return remote(src.at[tile_rows(m)], dst.at[tile_rows(m)], mate_send.at[1 + k, m], mate_f.at[k, m], mate)

    def forward(m, carry):
        at = tile_rows(m)

        @pl.when(s > 0)
        def _():
            forward_copy(m, (at,)).wait_recv()

        saved_copy(0, m).start()
        values = arriving[at, :].astype(F32)
        q = lax.rsqrt(jnp.sum(values * values, axis=-1, keepdims=True) * (1.0 / width) + epsilon)
        scale[at, :] = jnp.broadcast_to(q, (rows, 128))
        normal = (values * q * gain_ref[...]).astype(BF)
        for c in range(chunks):
            cols = pl.ds(c * chunk, chunk)
            p = jnp.dot(normal, w[:, cols], preferred_element_type=F32)
            cdf = 0.5 * (1.0 + lax.erf(p * half_root))
            leaving[at, cols] = (arriving[at, cols].astype(F32) + p * cdf).astype(BF)

            @pl.when(s < last)
            def _():
                forward_copy(m, (at, cols)).start()

            preact[at, cols] = p.astype(BF)
            slope[at, cols] = (cdf + p * (jnp.exp(-0.5 * p * p) * density_scale)).astype(BF)
        for k in (1, 2, 3):
            saved_copy(k, m).start()
        low = lax.broadcasted_iota(jnp.int32, (rows, 128), 1) < 64
        for k in range(width // 256):
            first = arriving[at, pl.ds(256 * k, 128)].astype(F32) * q * gain_ref[:, pl.ds(256 * k, 128)]
            second = arriving[at, pl.ds(256 * k + 128, 128)].astype(F32) * q * gain_ref[:, pl.ds(256 * k + 128, 128)]
            cols = pl.ds(128 * k, 128)
            theirs[at, cols] = jnp.where(low, first, pltpu.roll(second, 64, 1)).astype(BF)
            mine[at, cols] = jnp.where(low, pltpu.roll(first, 64, 1), second).astype(BF)
        half_copy(m).start()
        return carry

    def backward(m, carry):
        at = tile_rows(m)
        for k in (0, 1, 2, 3):
            saved_copy(k, m).wait_recv()

        @pl.when(s < last)
        def _():
            backward_copy(m, (at,)).wait_recv()

        gp = (arriving[at, :].astype(F32) * slope[at, :].astype(F32)).astype(BF)
        grad_pre[at, :] = gp
        grad_copy(m).start()

        @pl.when(s > 0)
        def _():
            q = scale[at, 0:1]
            mean = jnp.sum(gp.astype(F32) * preact[at, :].astype(F32), axis=-1, keepdims=True) * (1.0 / width)
            pull = q * q * mean
            for c in range(chunks):
                cols = pl.ds(c * chunk, chunk)
                a = jnp.dot(gp, turned[:, cols], preferred_element_type=F32)
                a = a * gain_ref[:, cols]
                leaving[at, cols] = (arriving[at, cols].astype(F32) + q * a - hidden[at, cols].astype(F32) * pull).astype(BF)
                backward_copy(m, (at, cols)).start()
        return carry

    def received_grad(m, carry):
        grad_copy(m).wait_recv()
        return carry

    def received_half(m, carry):
        half_copy(m).wait_recv()
        return carry

    @pl.when(forward_core)
    def _():
        @pl.when(s == 0)
        def _():
            x_copy.wait()
            x_mate.wait_recv()

        lax.fori_loop(0, micros, forward, 0)
        lax.fori_loop(0, micros, received_grad, 0)

    @pl.when(backward_core)
    def _():
        def turn(i, carry):
            at = pl.ds(pl.multiple_of(i * 128, 128), 128)
            turned[:, at] = w[at, :].T
            return carry

        lax.fori_loop(0, width // 128, turn, 0)

        @pl.when(s == last)
        def _():
            ct_copy.wait()
            ct_mate.wait_recv()

        lax.fori_loop(0, micros, backward, 0)
        lax.fori_loop(0, micros, received_half, 0)

    flip_copy(9, 5, right2).wait_recv()
    flip_copy(5, 7, right2).start()

    def terms(i, carry):
        cols = pl.ds(pl.multiple_of(i * 256, 256), 256)
        part[cols, :] = lax.dot_general(
            mine[:, cols], grad_pre[...], (((0,), (0,)), ((), ())), preferred_element_type=F32).astype(BF)
        return carry

    lax.fori_loop(0, half_width // 256, terms, 0)

    def block(r1, r2):
        return pl.ds(pl.multiple_of(chip(core, r1, r2) * shard, shard), shard)

    def slot(r2, count=1):
        return pl.ds(r2 * shard, count * shard)

    def first_ring(src_r1, r2, d, dst, dst_slot, recv):
        return remote(part.at[block(src_r1, r2)], dst.at[dst_slot], rs_send.at[d], recv, around[d])

    toward_left, toward_right = (2, 1), (3, 0)
    for r2 in toward_left:
        first_ring(2, r2, 1, part_a, slot(r2), a_recv.at[r2]).start()
    for r2 in toward_right:
        first_ring(2, r2, 0, part_a, slot(r2), a_recv.at[r2]).start()
    for r2 in toward_right:
        first_ring(3, r2, 1, part_b, slot(r2), ab_recv.at[0, r2]).start()
    for r2 in toward_left:
        first_ring(1, r2, 0, part_b, slot(4 + r2), ab_recv.at[1, r2]).start()
    for k in range(2):
        for r2, r1, d, side in ((toward_left[k], 3, 1, 0), (toward_right[k], 1, 0, 1)):
            first_ring(2, r2, d, part_a, slot(r2), a_recv.at[r2]).wait_recv()
            at = block(r1, r2)
            part[at, :] = (part[at, :].astype(F32) + part_a[slot(r2), :].astype(F32)).astype(BF)
            first_ring(r1, r2, d, part_b, slot(4 * side + r2), ab_recv.at[side, r2]).start()

    flip_copy(9, 6, left2).wait_recv()
    flip_copy(5, 7, right2).wait_recv()
    all_flips = flips[9] + flips[5] + flips[6] + flips[7]
    flip_ref[0] = jnp.sum(all_flips.astype(F32)).astype(jnp.int32)

    def ring_total(r2):
        for side in range(2):
            first_ring(3, r2, 1, part_b, slot(4 * side + r2), ab_recv.at[side, r2]).wait_recv()
        total = part[block(0, r2), :].astype(F32) + part_b[slot(r2), :].astype(F32) + part_b[slot(4 + r2), :].astype(F32)
        row_sum[slot(r2), :] = total.astype(BF)

    half = shard // 2

    def second_ring(r2, h, d, dst, start, recv):
        return remote(row_sum.at[pl.ds(r2 * shard + h * half, half)], dst.at[pl.ds(start, half)], rs_send.at[d], recv,
                      around[d])

    ring_total(2)
    second_ring(2, 0, 3, row_a, 0, ra_recv.at[0]).start()
    second_ring(2, 1, 2, row_a, half, ra_recv.at[1]).start()
    ring_total(3)
    second_ring(3, 1, 3, row_b, half, rb_recv.at[0, 1]).start()
    ring_total(1)
    second_ring(1, 0, 2, row_b, shard, rb_recv.at[1, 0]).start()
    for h, r2, d, side in ((0, 3, 3, 0), (1, 1, 2, 1)):
        second_ring(2, h, d, row_a, h * half, ra_recv.at[h]).wait_recv()
        at = pl.ds(r2 * shard + h * half, half)
        row_sum[at, :] = (row_sum[at, :].astype(F32) + row_a[pl.ds(h * half, half), :].astype(F32)).astype(BF)
        second_ring(r2, h, d, row_b, side * shard + h * half, rb_recv.at[side, h]).start()
    ring_total(0)
    for side, h in ((0, 1), (1, 0), (0, 0), (1, 1)):
        second_ring(2, h, 3, row_b, side * shard + h * half, rb_recv.at[side, h]).wait_recv()
    for k in range(width // piece):
        cols = pl.ds(k * piece, piece)
        total = row_sum[slot(0), cols].astype(F32) + row_b[slot(0), cols].astype(F32) + row_b[slot(1), cols].astype(F32)
        out_ref[:, cols] = total * (1.0 / math.sqrt(token_total)) + decay[k]

    def drain_forward(m, carry):
        @pl.when(s < last)
        def _():
            forward_copy(m, (tile_rows(m),)).wait_send()

        half_copy(m).wait_send()
        for k in range(4):
            saved_copy(k, m).wait_send()
        return carry

    def drain_backward(m, carry):
        @pl.when(s > 0)
        def _():
            backward_copy(m, (tile_rows(m),)).wait_send()

        grad_copy(m).wait_send()
        return carry

    @pl.when(forward_core)
    def _():
        lax.fori_loop(0, micros, drain_forward, 0)

        @pl.when(s == last)
        def _():
            ct_mate.wait_send()

    @pl.when(backward_core)
    def _():
        lax.fori_loop(0, micros, drain_backward, 0)

        @pl.when(s == 0)
        def _():
            x_mate.wait_send()

    def sent(sem, count):
        ref = grad_pre.at[pl.ds(0, count)]
        remote(ref, ref, sem, flip_recv.at[0], mate).wait_send()

    for d in (0, 1):
        sent(ag_send.at[d], 3 * groups)
    for d in (2, 3):
        sent(ag_send.at[d], 12 * groups)
    sent(ag_send.at[4], 2 * BLOCKS * groups)
    for d in (0, 1):
        sent(rs_send.at[d], 6 * shard)
    for d in (2, 3):
        sent(rs_send.at[d], 3 * half)
    for dst in range(1, 8):
        flip_copy(0, dst, mate).wait_send()


def step(x, ct, weight, gain, pair, earlier, sections, token_total, micros):
    rows, width = x.shape
    shard = weight.shape[0]
    groups = shard // 4
    vmem = pl.BlockSpec(memory_space=pltpu.VMEM)
    hbm = pl.BlockSpec(memory_space=pl.ANY)
    act = pltpu.VMEM((2 * rows, width), BF)
    dma = pltpu.SemaphoreType.DMA
    return pl.pallas_call(
        functools.partial(kernel, micros, sections, token_total),
        out_shape=(jax.ShapeDtypeStruct((shard, width), F32), jax.ShapeDtypeStruct((1,), jnp.int32)),
        in_specs=[hbm, hbm, vmem, vmem, hbm, vmem],
        out_specs=(vmem, pl.BlockSpec(memory_space=pltpu.SMEM)),
        scratch_shapes=[
            pltpu.VMEM((width, width), BF),
            pltpu.VMEM((width, width), BF),
            pltpu.VMEM((2 * BLOCKS, 2 * groups, width), BF),
            pltpu.VMEM(pair.shape, jnp.int32),
            pltpu.VMEM((width // 128, shard, 128), F32),
            pltpu.VMEM((width // 128, shard, 128), F32),
            act, act, act, act, act, pltpu.VMEM((2 * rows, 128), F32),
            pltpu.VMEM((2 * rows, width // 2), BF),
            pltpu.VMEM((2 * rows, width // 2), BF),
            pltpu.VMEM((2 * rows, width), BF),
            pltpu.VMEM((width // 2, width), BF),
            pltpu.VMEM((SIDE * shard, width), BF),
            pltpu.VMEM((2 * SIDE * shard, width), BF),
            pltpu.VMEM((SIDE * shard, width), BF),
            pltpu.VMEM((shard, width), BF),
            pltpu.VMEM((2 * shard, width), BF),
            pltpu.VMEM((10, 8, 128), jnp.int32),
            dma((2,)), dma((5,)), dma((BLOCKS, 2)), dma((BLOCKS,)), dma((1,)), dma((1,)),
            dma((micros,)), dma((micros,)), dma((micros,)), dma((micros,)), dma((4, micros)), dma((5, micros)),
            dma((SIDE,)), dma((2, SIDE)), dma((2,)), dma((2, 2)), dma((4,)), dma((7,)), dma((7,)),
        ],
        compiler_params=pltpu.CompilerParams(
            collective_id=0, has_side_effects=True, vmem_limit_bytes=58 * 1024 * 1024),
    )(x, ct, weight, gain, pair, earlier)


def body(activations, cotangent, weight, norm_gain, pair_mask, earlier_mask):
    micro_count, row_count, model_width = activations.shape
    tokens = micro_count * row_count
    gradient, flip_sum = step(
        activations.reshape(tokens, model_width), cotangent.reshape(tokens, model_width), weight[0], norm_gain,
        pair_mask[0], earlier_mask[0], lax.axis_size("section"), tokens * lax.axis_size("dp"), 16)
    return (gradient[None], flip_sum)


def solution(mesh):
    placed = (
        P(None, "dp", None),
        P(None, "dp", None),
        P("section", "dp", None),
        P("section", None),
        P("section", None, None),
        P("section", "dp", None),
    )
    return jax.shard_map(
        body,
        mesh=mesh,
        in_specs=placed,
        out_specs=(P("section", "dp", None), P("section")),
        check_vma=False,
    )
```

```python
import functools
import math

import jax
import jax.numpy as jnp
from jax import lax
from jax.experimental import pallas as pl
from jax.experimental.pallas import tpu as pltpu
from jax.sharding import PartitionSpec as P

MESH = pl.DeviceIdType.MESH
epsilon = 1e-06
decay_rate = 4.0
half_root = 0.7071067811865476
density_scale = 0.3989422804014327
BF = jnp.bfloat16
F32 = jnp.float32
SIDE = 4
CHUNK = 1024
BLOCKS = SIDE * SIDE


def kernel(sections, token_total, x_hbm, ct_hbm, weight_hbm, gain_hbm, pair_hbm, earlier_hbm, out_ref, flip_ref,
           weight_ref, gain_ref, earlier_ref, own_pairs, first_sem,
           w, turned, packed, pair, wide_rows, decay, arriving, leaving, hidden, preact, slope, scale, mine, theirs,
           grad_pre, part, part_a, part_b, row_sum, row_a, row_b, flips,
           local_sem, ag_send, ag_recv, far_recv, mate_recv, in_send, in_recv, z_send, z_recv, mate_n, mate_g, mate_f, mate_send,
           a_recv, ab_recv, ra_recv, rb_recv, rs_send, flip_send, flip_recv):
    s = lax.axis_index("section")
    dp = lax.axis_index("dp")
    core, xx, yy = dp % 2, (dp // 2) % SIDE, dp // (2 * SIDE)
    last = sections - 1
    micros, chunks, rows, chunk = arriving.shape
    width = chunks * chunk
    ahead = pl.ds(0, micros // 2), pl.ds(micros // 2, micros // 2)
    forward_core, backward_core = core == 1, core == 0
    shard = weight_ref.shape[0]
    groups = shard // 4
    half_width = width // 2

    def chip(plane, r1, r2):
        dx, dy = jnp.where(plane == 0, r1, r2), jnp.where(plane == 0, r2, r1)
        return ((yy + dy) % SIDE) * SIDE + (xx + dx) % SIDE

    mate = 2 * (dp // 2) + (1 - core)
    right1, left1 = 2 * chip(core, 1, 0) + core, 2 * chip(core, 3, 0) + core
    right2, left2 = 2 * chip(core, 0, 1) + core, 2 * chip(core, 0, 3) + core
    around = (right1, left1, right2, left2)

    def remote(src, dst, send, recv, target):
        return pltpu.make_async_remote_copy(
            src_ref=src, dst_ref=dst, send_sem=send, recv_sem=recv, device_id={"dp": target}, device_id_type=MESH)

    own_groups = pl.ds(pl.multiple_of(dp * groups, groups), groups)
    first_copies = (
        pltpu.make_async_copy(pair_hbm.at[own_groups], own_pairs, first_sem.at[0]),
        pltpu.make_async_copy(weight_hbm, weight_ref, first_sem.at[1]),
        pltpu.make_async_copy(earlier_hbm, earlier_ref, first_sem.at[2]),
        pltpu.make_async_copy(gain_hbm, gain_ref, first_sem.at[3]),
    )
    for copy in first_copies:
        copy.start()
    pair_copy = pltpu.make_async_copy(pair_hbm, pair, local_sem.at[0])
    pair_copy.start()
    pieces = [pl.ds(c * chunk, chunk) for c in range(chunks)]
    x_copies = [pltpu.make_async_copy(x_hbm.at[:, :, cols], arriving.at[ahead[0], c], local_sem.at[1 + c])
                for c, cols in enumerate(pieces)]
    ct_copies = [pltpu.make_async_copy(ct_hbm.at[:, :, cols], arriving.at[ahead[1], c], local_sem.at[1 + c])
                 for c, cols in enumerate(pieces)]
    x_mates = [remote(x_hbm.at[:, :, cols], arriving.at[ahead[1], c], in_send.at[c], in_recv.at[c], mate)
               for c, cols in enumerate(pieces)]
    ct_mates = [remote(ct_hbm.at[:, :, cols], arriving.at[ahead[0], c], in_send.at[c], in_recv.at[c], mate)
                for c, cols in enumerate(pieces)]

    @pl.when((s == 0) & forward_core)
    def _():
        for copy in x_copies:
            copy.start()

    @pl.when((s == last) & backward_core)
    def _():
        for copy in ct_copies:
            copy.start()

    barrier = pltpu.get_barrier_semaphore()
    for target in (*around, mate):
        pl.semaphore_signal(barrier, inc=1, device_id={"dp": target}, device_id_type=MESH)

    @pl.when(s > 0)
    def _():
        pl.semaphore_signal(barrier, inc=1, device_id={"section": s - 1}, device_id_type=MESH)

    @pl.when(s < last)
    def _():
        pl.semaphore_signal(barrier, inc=1, device_id={"section": s + 1}, device_id_type=MESH)

    piece = 128
    for copy in first_copies:
        copy.wait()
    counted = jnp.zeros((8, 128), jnp.int32)
    for k in range(width // piece):
        cols = pl.ds(k * piece, piece)
        p = own_pairs[:, cols]
        wide_rows[k] = weight_ref[:, cols].astype(F32)
        w0, w1, w2, w3 = (wide_rows[k, pl.ds(j, groups, stride=4), :] for j in range(4))
        lead = jnp.where(p < 3, w0, jnp.where(p == 5, w2, w1))
        trail = jnp.where(p == 0, w1, jnp.where((p == 1) | (p == 3), w2, w3))
        packed[dp, 0:groups, cols] = lead.astype(BF)
        packed[dp, groups:2 * groups, cols] = trail.astype(BF)
        kept = (p < 3, (p == 0) | (p == 3) | (p == 4), (p == 1) | (p == 3) | (p == 5), (p == 2) | (p > 3))
        for j, (k_j, w_j) in enumerate(zip(kept, (w0, w1, w2, w3))):
            decay[k, pl.ds(j, groups, stride=4), :] = jnp.where(k_j, 0.0, decay_rate * w_j)
        e = earlier_ref[:, cols]
        changed = jnp.where(p == e, 0, jnp.where(p + e == 5, 4, 2))
        for a in range(groups // 8):
            for b in range(piece // 128):
                counted = counted + changed[8 * a:8 * a + 8, 128 * b:128 * b + 128]
    flips[0] = counted

    pl.semaphore_wait(barrier, 5 + jnp.where(s > 0, 1, 0) + jnp.where(s < last, 1, 0))

    @pl.when((s == 0) & backward_core)
    def _():
        for copy in x_mates:
            copy.start()

    @pl.when((s == last) & forward_core)
    def _():
        for copy in ct_mates:
            copy.start()

    def shard_copy(b, d, recv):
        ref = packed.at[2 * b + core]
        return remote(ref, ref, ag_send.at[d], recv, (*around, mate)[d])

    def send_shard(b, d):
        shard_copy(b, d, ag_recv.at[b]).start()

    def wait_shard(b):
        shard_copy(b, 0, ag_recv.at[b]).wait_recv()

    def half_shard(b, h):
        ref = packed.at[2 * b + core, pl.ds(h * groups, groups)]
        return remote(ref, ref, ag_send.at[h], far_recv.at[h], around[h])

    def send_mate(b):
        shard_copy(b, 4, mate_recv.at[b]).start()

    def wait_mate(b):
        slot = 2 * b + (1 - core)
        remote(packed.at[slot], packed.at[slot], ag_send.at[4], mate_recv.at[b], mate).wait_recv()

    def spread(b):
        send_shard(b, 2)
        send_shard(b, 3)
        send_mate(b)

    def unpack(slot):
        at = pl.ds(pl.multiple_of(slot * groups, groups), groups)
        to = pl.ds(pl.multiple_of(slot * shard, shard), shard)
        for k in range(width // piece):
            cols = pl.ds(k * piece, piece)
            p = pair[at, cols]
            lead = packed[slot, 0:groups, cols].astype(F32)
            trail = packed[slot, groups:2 * groups, cols].astype(F32)
            o0 = jnp.where(p < 3, lead, 0.0)
            o1 = jnp.where(p == 0, trail, jnp.where((p == 3) | (p == 4), lead, 0.0))
            o2 = jnp.where(p == 5, lead, jnp.where((p == 1) | (p == 3), trail, 0.0))
            o3 = jnp.where((p == 2) | (p > 3), trail, 0.0)
            for j, o in enumerate((o0, o1, o2, o3)):
                wide_rows[k, pl.ds(j, groups, stride=4), :] = o
            w[to, cols] = wide_rows[k].astype(BF)

    def flip_copy(src, dst, target):
        return remote(flips.at[src], flips.at[dst], flip_send.at[dst - 1], flip_recv.at[dst - 1], target)

    own = chip(core, 0, 0)
    send_shard(own, 0)
    send_shard(own, 1)
    spread(own)
    flip_copy(0, 1, mate).start()
    pair_copy.wait()
    unpack(dp)
    from_left, from_right, far = chip(core, 3, 0), chip(core, 1, 0), chip(core, 2, 0)
    wait_shard(from_left)
    half_shard(from_left, 0).start()
    spread(from_left)
    wait_shard(from_right)
    half_shard(from_right, 1).start()
    spread(from_right)
    flip_copy(0, 1, mate).wait_recv()
    flips[8] = flips[0] + flips[1]
    flip_copy(8, 2, right1).start()
    flip_copy(8, 3, left1).start()
    unpack(2 * from_left + core)
    half_shard(far, 0).wait_recv()
    half_shard(far, 1).wait_recv()
    spread(far)

    def near(i, carry):
        r1 = jnp.where(i == 0, 0, jnp.where(i == 1, 3, jnp.where(i == 2, 1, 2)))
        lower, upper = chip(core, r1, 3), chip(core, r1, 1)
        wait_shard(lower)

        @pl.when(i < 2)
        def _():
            send_shard(lower, 2)

        send_mate(lower)
        wait_shard(upper)

        @pl.when(i >= 2)
        def _():
            send_shard(upper, 3)

        send_mate(upper)
        other = chip(1 - core, r1, 0)
        wait_mate(other)

        def expand(j, c):
            unpack(jnp.where(j == 0, 2 * other + (1 - core), jnp.where(j == 1, 2 * lower + core, 2 * upper + core)))
            return c

        lax.fori_loop(0, 3, expand, 0)
        return carry

    lax.fori_loop(0, SIDE, near, 0)

    def expand_rest(j, c):
        unpack(2 * jnp.where(j == 0, from_right, far) + core)
        return c

    lax.fori_loop(0, 2, expand_rest, 0)
    flip_copy(8, 2, right1).wait_recv()
    flip_copy(2, 4, right1).start()

    def distant(i, carry):
        r1 = jnp.where(i == 0, 0, jnp.where(i == 1, 3, jnp.where(i == 2, 1, 2)))
        beyond = chip(core, r1, 2)
        wait_shard(beyond)
        send_mate(beyond)
        lower, upper = chip(1 - core, r1, 3), chip(1 - core, r1, 1)
        wait_mate(lower)
        wait_mate(upper)

        def expand(j, c):
            unpack(jnp.where(j == 0, 2 * beyond + core,
                             jnp.where(j == 1, 2 * lower + (1 - core), 2 * upper + (1 - core))))
            return c

        lax.fori_loop(0, 3, expand, 0)
        return carry

    lax.fori_loop(0, SIDE, distant, 0)

    def final(i, carry):
        r1 = jnp.where(i == 0, 0, jnp.where(i == 1, 3, jnp.where(i == 2, 1, 2)))
        b = chip(1 - core, r1, 2)
        wait_mate(b)
        unpack(2 * b + (1 - core))
        return carry

    lax.fori_loop(0, SIDE, final, 0)

    flip_copy(8, 3, left1).wait_recv()
    flip_copy(2, 4, right1).wait_recv()
    flips[9] = flips[8] + flips[2] + flips[3] + flips[4]
    flip_copy(9, 5, right2).start()
    flip_copy(9, 6, left2).start()

    def tile_rows(m):
        return pl.ds(pl.multiple_of(m * rows, rows), rows)

    def z_copy(m, where, target):
        return pltpu.make_async_remote_copy(
            src_ref=leaving.at[where], dst_ref=arriving.at[where], send_sem=z_send.at[m], recv_sem=z_recv.at[m],
            device_id={"section": target}, device_id_type=MESH)

    def forward_copy(m, *where):
        return z_copy(m, (m, *where), jnp.minimum(s + 1, last))

    def backward_copy(m, *where):
        return z_copy(m, (m, *where), jnp.maximum(s - 1, 0))

    def half_copy(m):
        return remote(theirs.at[tile_rows(m)], mine.at[tile_rows(m)], mate_send.at[0, m], mate_n.at[m], mate)

    def grad_copy(m):
        return remote(grad_pre.at[tile_rows(m)], grad_pre.at[tile_rows(m)], mate_send.at[0, m], mate_g.at[m], mate)

    def saved_copy(k, m):
        src = (arriving, slope, preact, scale)[k]
        dst = (hidden, slope, preact, scale)[k]
        at = m if k == 0 else tile_rows(m)
        return remote(src.at[at], dst.at[at], mate_send.at[1 + k, m], mate_f.at[k, m], mate)

    def forward(m, carry):
        at = tile_rows(m)

        @pl.when(s > 0)
        def _():
            forward_copy(m).wait_recv()

        saved_copy(0, m).start()
        gained, squares = [], 0.0
        for c, cols in enumerate(pieces):
            values = arriving[m, c].astype(F32)
            gained.append((values * gain_ref[:, cols]).astype(BF))
            squares += jnp.sum(values * values, axis=-1, keepdims=True)
        gained = jnp.concatenate(gained, axis=1)
        q = lax.rsqrt(squares * (1.0 / width) + epsilon)
        scale[at, :] = jnp.broadcast_to(q, (rows, 128))
        for c, cols in enumerate(pieces):
            p = jnp.dot(gained, w[:, cols], preferred_element_type=F32) * q
            cdf = 0.5 * (1.0 + lax.erf(p * half_root))
            leaving[m, c] = (arriving[m, c].astype(F32) + p * cdf).astype(BF)

            @pl.when(s < last)
            def _():
                forward_copy(m, c).start()

            preact[at, cols] = p.astype(BF)
            slope[at, cols] = (cdf + p * (jnp.exp(-0.5 * p * p) * density_scale)).astype(BF)
        for k in (1, 2, 3):
            saved_copy(k, m).start()
        return carry

    def halves(m, carry):
        at = tile_rows(m)
        q = scale[at, :]
        low = lax.broadcasted_iota(jnp.int32, (rows, 128), 1) < 64

        def scaled(start):
            values = arriving[m, start // chunk, :, pl.ds(start % chunk, 128)].astype(F32)
            return values * q * gain_ref[:, pl.ds(start, 128)]

        for k in range(width // 256):
            first, second = scaled(256 * k), scaled(256 * k + 128)
            cols = pl.ds(128 * k, 128)
            mine[at, cols] = jnp.where(low, pltpu.roll(first, 64, 1), second).astype(BF)
        for k in range(width // 256):
            start = (k % 2) * 1024 + (k // 2) * 128
            first, second = scaled(start), scaled(start + 512)
            theirs[at, pl.ds(128 * k, 128)] = jnp.where(low, first, pltpu.roll(second, 64, 1)).astype(BF)
        half_copy(m).start()
        return carry

    def backward(m, carry):
        at = tile_rows(m)
        for k in (0, 1, 2, 3):
            saved_copy(k, m).wait_recv()

        @pl.when(s < last)
        def _():
            backward_copy(m).wait_recv()

        gp = jnp.concatenate(
            [(arriving[m, c].astype(F32) * slope[at, cols].astype(F32)).astype(BF) for c, cols in enumerate(pieces)],
            axis=1)
        grad_pre[at, :] = gp
        grad_copy(m).start()

        @pl.when(s > 0)
        def _():
            q = scale[at, 0:1]
            mean = jnp.sum(gp.astype(F32) * preact[at, :].astype(F32), axis=-1, keepdims=True) * (1.0 / width)
            pull = q * q * mean
            for c, cols in enumerate(pieces):
                a = jnp.dot(gp, turned[:, cols], preferred_element_type=F32)
                a = a * gain_ref[:, cols]
                leaving[m, c] = (arriving[m, c].astype(F32) + q * a - hidden[m, c].astype(F32) * pull).astype(BF)
                backward_copy(m, c).start()
        return carry

    def received_grad(m, carry):
        grad_copy(m).wait_recv()
        return carry

    def received_half(m, carry):
        half_copy(m).wait_recv()
        return carry

    @pl.when(forward_core)
    def _():
        @pl.when(s == 0)
        def _():
            for copy in x_copies:
                copy.wait()
            for copy in x_mates:
                copy.wait_recv()

        lax.fori_loop(0, micros, forward, 0)
        lax.fori_loop(0, micros, halves, 0)
        lax.fori_loop(0, micros, received_grad, 0)

    @pl.when(backward_core)
    def _():
        def turn(i, carry):
            at = pl.ds(pl.multiple_of(i * 128, 128), 128)
            turned[:, at] = w[at, :].T
            return carry

        lax.fori_loop(0, width // 128, turn, 0)

        @pl.when(s == last)
        def _():
            for copy in ct_copies:
                copy.wait()
            for copy in ct_mates:
                copy.wait_recv()

        lax.fori_loop(0, micros, backward, 0)
        lax.fori_loop(0, micros, received_half, 0)

    flip_copy(9, 5, right2).wait_recv()
    flip_copy(5, 7, right2).start()

    place1, place2 = jnp.where(core == 0, xx, yy), jnp.where(core == 0, yy, xx)

    def block(r1, r2):
        place = ((place1 + r1) % SIDE) * SIDE + (place2 + r2) % SIDE
        return pl.ds(pl.multiple_of(place * shard, shard), shard)

    def terms(i):
        r1 = jnp.where(i == 0, 2, jnp.where(i == 1, 3, jnp.where(i == 2, 1, 0)))
        cols = pl.ds(pl.multiple_of(((place1 + r1) % SIDE) * (SIDE * shard), SIDE * shard), SIDE * shard)
        part[cols, :] = lax.dot_general(
            mine[:, cols], grad_pre[...], (((0,), (0,)), ((), ())), preferred_element_type=F32).astype(BF)

    def slot(r2, count=1):
        return pl.ds(r2 * shard, count * shard)

    def first_ring(src_r1, r2, d, dst, dst_slot, recv):
        return remote(part.at[block(src_r1, r2)], dst.at[dst_slot], rs_send.at[d], recv, around[d])

    toward_left, toward_right = (2, 1), (3, 0)
    def group(i, carry):
        terms(i)

        @pl.when(i == 0)
        def _():
            for k in range(2):
                first_ring(2, toward_left[k], 1, part_a, slot(toward_left[k]), a_recv.at[toward_left[k]]).start()
                first_ring(2, toward_right[k], 0, part_a, slot(toward_right[k]), a_recv.at[toward_right[k]]).start()

        @pl.when(i == 1)
        def _():
            for r2 in toward_right:
                first_ring(3, r2, 1, part_b, slot(r2), ab_recv.at[0, r2]).start()

        @pl.when(i == 2)
        def _():
            for r2 in toward_left:
                first_ring(1, r2, 0, part_b, slot(4 + r2), ab_recv.at[1, r2]).start()

        return carry

    lax.fori_loop(0, SIDE, group, 0)
    for k in range(2):
        for r2, r1, d, side in ((toward_left[k], 3, 1, 0), (toward_right[k], 1, 0, 1)):
            first_ring(2, r2, d, part_a, slot(r2), a_recv.at[r2]).wait_recv()
            at = block(r1, r2)
            part[at, :] = (part[at, :].astype(F32) + part_a[slot(r2), :].astype(F32)).astype(BF)
            first_ring(r1, r2, d, part_b, slot(4 * side + r2), ab_recv.at[side, r2]).start()

    flip_copy(9, 6, left2).wait_recv()
    flip_copy(5, 7, right2).wait_recv()
    all_flips = flips[9] + flips[5] + flips[6] + flips[7]
    flip_ref[0] = jnp.sum(all_flips.astype(F32)).astype(jnp.int32)

    def ring_total(r2):
        for side in range(2):
            first_ring(3, r2, 1, part_b, slot(4 * side + r2), ab_recv.at[side, r2]).wait_recv()
        total = part[block(0, r2), :].astype(F32) + part_b[slot(r2), :].astype(F32) + part_b[slot(4 + r2), :].astype(F32)
        row_sum[slot(r2), :] = total.astype(BF)

    half = shard // 2

    def second_ring(r2, h, d, dst, start, recv):
        return remote(row_sum.at[pl.ds(r2 * shard + h * half, half)], dst.at[pl.ds(start, half)], rs_send.at[d], recv,
                      around[d])

    ring_total(2)
    second_ring(2, 0, 3, row_a, 0, ra_recv.at[0]).start()
    second_ring(2, 1, 2, row_a, half, ra_recv.at[1]).start()
    ring_total(3)
    second_ring(3, 1, 3, row_b, half, rb_recv.at[0, 1]).start()
    ring_total(1)
    second_ring(1, 0, 2, row_b, shard, rb_recv.at[1, 0]).start()
    for h, r2, d, side in ((0, 3, 3, 0), (1, 1, 2, 1)):
        second_ring(2, h, d, row_a, h * half, ra_recv.at[h]).wait_recv()
        at = pl.ds(r2 * shard + h * half, half)
        row_sum[at, :] = (row_sum[at, :].astype(F32) + row_a[pl.ds(h * half, half), :].astype(F32)).astype(BF)
        second_ring(r2, h, d, row_b, side * shard + h * half, rb_recv.at[side, h]).start()
    ring_total(0)
    for side, h in ((0, 1), (1, 0), (0, 0), (1, 1)):
        second_ring(2, h, 3, row_b, side * shard + h * half, rb_recv.at[side, h]).wait_recv()
    for k in range(width // piece):
        cols = pl.ds(k * piece, piece)
        total = row_sum[slot(0), cols].astype(F32) + row_b[slot(0), cols].astype(F32) + row_b[slot(1), cols].astype(F32)
        out_ref[:, cols] = total * (1.0 / math.sqrt(token_total)) + decay[k]

    def drain_forward(m, carry):
        @pl.when(s < last)
        def _():
            forward_copy(m).wait_send()

        half_copy(m).wait_send()
        for k in range(4):
            saved_copy(k, m).wait_send()
        return carry

    def drain_backward(m, carry):
        @pl.when(s > 0)
        def _():
            backward_copy(m).wait_send()

        grad_copy(m).wait_send()
        return carry

    @pl.when(forward_core)
    def _():
        lax.fori_loop(0, micros, drain_forward, 0)

        @pl.when(s == last)
        def _():
            for copy in ct_mates:
                copy.wait_send()

    @pl.when(backward_core)
    def _():
        lax.fori_loop(0, micros, drain_backward, 0)

        @pl.when(s == 0)
        def _():
            for copy in x_mates:
                copy.wait_send()

    def sent(sem, count):
        ref = grad_pre.at[pl.ds(0, count)]
        remote(ref, ref, sem, flip_recv.at[0], mate).wait_send()

    for d in (0, 1):
        sent(ag_send.at[d], 3 * groups)
    for d in (2, 3):
        sent(ag_send.at[d], 12 * groups)
    sent(ag_send.at[4], 2 * BLOCKS * groups)
    for d in (0, 1):
        sent(rs_send.at[d], 6 * shard)
    for d in (2, 3):
        sent(rs_send.at[d], 3 * half)
    for dst in range(1, 8):
        flip_copy(0, dst, mate).wait_send()


def step(x, ct, weight, gain, pair, earlier, sections, token_total, chunk):
    micros, tall, width = x.shape
    micros, rows = 2 * micros, micros * tall
    chunks = width // chunk
    shard = weight.shape[0]
    groups = shard // 4
    vmem = pl.BlockSpec(memory_space=pltpu.VMEM)
    hbm = pl.BlockSpec(memory_space=pl.ANY)
    act = pltpu.VMEM((2 * rows, width), BF)
    stream = pltpu.VMEM((micros, chunks, tall, chunk), BF)
    dma = pltpu.SemaphoreType.DMA
    return pl.pallas_call(
        functools.partial(kernel, sections, token_total),
        out_shape=(jax.ShapeDtypeStruct((shard, width), F32), jax.ShapeDtypeStruct((1,), jnp.int32)),
        in_specs=[hbm] * 6,
        out_specs=(vmem, pl.BlockSpec(memory_space=pltpu.SMEM)),
        scratch_shapes=[
            pltpu.VMEM((shard, width), BF), pltpu.VMEM((1, width), F32), pltpu.VMEM((groups, width), jnp.int32),
            pltpu.VMEM((groups, width), jnp.int32), dma((4,)),
            pltpu.VMEM((width, width), BF),
            pltpu.VMEM((width, width), BF),
            pltpu.VMEM((2 * BLOCKS, 2 * groups, width), BF),
            pltpu.VMEM(pair.shape, jnp.int32),
            pltpu.VMEM((width // 128, shard, 128), F32),
            pltpu.VMEM((width // 128, shard, 128), F32),
            stream, stream, stream, act, act, pltpu.VMEM((2 * rows, 128), F32),
            pltpu.VMEM((2 * rows, width // 2), BF),
            pltpu.VMEM((2 * rows, width // 2), BF),
            pltpu.VMEM((2 * rows, width), BF),
            pltpu.VMEM((width // 2, width), BF),
            pltpu.VMEM((SIDE * shard, width), BF),
            pltpu.VMEM((2 * SIDE * shard, width), BF),
            pltpu.VMEM((SIDE * shard, width), BF),
            pltpu.VMEM((shard, width), BF),
            pltpu.VMEM((2 * shard, width), BF),
            pltpu.VMEM((10, 8, 128), jnp.int32),
            dma((1 + chunks,)), dma((5,)), dma((BLOCKS,)), dma((2,)), dma((BLOCKS,)), dma((chunks,)), dma((chunks,)),
            dma((micros,)), dma((micros,)), dma((micros,)), dma((micros,)), dma((4, micros)), dma((5, micros)),
            dma((SIDE,)), dma((2, SIDE)), dma((2,)), dma((2, 2)), dma((4,)), dma((7,)), dma((7,)),
        ],
        compiler_params=pltpu.CompilerParams(
            collective_id=0, has_side_effects=True, vmem_limit_bytes=58 * 1024 * 1024),
    )(x, ct, weight, gain, pair, earlier)


def body(activations, cotangent, weight, norm_gain, pair_mask, earlier_mask):
    micro_count, row_count, model_width = activations.shape
    tokens = micro_count * row_count
    tall = 32
    gradient, flip_sum = step(
        activations.reshape(tokens // tall, tall, model_width), cotangent.reshape(tokens // tall, tall, model_width),
        weight[0], norm_gain, pair_mask[0], earlier_mask[0], lax.axis_size("section"),
        tokens * lax.axis_size("dp"), CHUNK)
    return (gradient[None], flip_sum)


def solution(mesh):
    placed = (
        P(None, "dp", None),
        P(None, "dp", None),
        P("section", "dp", None),
        P("section", None),
        P("section", None, None),
        P("section", "dp", None),
    )
    return jax.shard_map(
        body,
        mesh=mesh,
        in_specs=placed,
        out_specs=(P("section", "dp", None), P("section")),
        check_vma=False,
    )
```

```python
import functools
import math

import jax
import jax.numpy as jnp
from jax import lax
from jax.experimental import pallas as pl
from jax.experimental.pallas import tpu as pltpu
from jax.sharding import PartitionSpec as P

MESH = pl.DeviceIdType.MESH
epsilon = 1e-06
decay_rate = 4.0
half_root = 0.7071067811865476
density_scale = 0.3989422804014327
BF = jnp.bfloat16
F32 = jnp.float32
SIDE = 4
CHUNK = 1024
TAIL = 3
BLOCKS = SIDE * SIDE


def kernel(sections, token_total, x_hbm, ct_hbm, weight_hbm, gain_hbm, pair_hbm, earlier_hbm, out_ref, flip_ref,
           weight_ref, gain_ref, earlier_ref, own_pairs, first_sem,
           w, turned, packed, pair, wide_rows, decay, arriving, leaving, hidden, tail_out, t_send, t_recv, preact, slope, scale, mine, theirs,
           grad_pre, part, part_a, part_b, row_sum, row_a, row_b, flips,
           local_sem, ag_send, ag_recv, far_recv, mate_recv, in_send, in_recv, z_send, z_recv, mate_n, mate_g, mate_f, mate_send,
           a_recv, ab_recv, ra_recv, rb_recv, rs_send, flip_send, flip_recv):
    s = lax.axis_index("section")
    dp = lax.axis_index("dp")
    core, xx, yy = dp % 2, (dp // 2) % SIDE, dp // (2 * SIDE)
    last = sections - 1
    micros, chunks, rows, chunk = arriving.shape
    width = chunks * chunk
    early = micros - TAIL
    ahead = pl.ds(0, micros // 2), pl.ds(micros // 2, micros // 2)
    forward_core, backward_core = core == 1, core == 0
    shard = weight_ref.shape[0]
    groups = shard // 4
    half_width = width // 2

    def chip(plane, r1, r2):
        dx, dy = jnp.where(plane == 0, r1, r2), jnp.where(plane == 0, r2, r1)
        return ((yy + dy) % SIDE) * SIDE + (xx + dx) % SIDE

    mate = 2 * (dp // 2) + (1 - core)
    right1, left1 = 2 * chip(core, 1, 0) + core, 2 * chip(core, 3, 0) + core
    right2, left2 = 2 * chip(core, 0, 1) + core, 2 * chip(core, 0, 3) + core
    around = (right1, left1, right2, left2)

    def remote(src, dst, send, recv, target):
        return pltpu.make_async_remote_copy(
            src_ref=src, dst_ref=dst, send_sem=send, recv_sem=recv, device_id={"dp": target}, device_id_type=MESH)

    own_groups = pl.ds(pl.multiple_of(dp * groups, groups), groups)
    first_copies = (
        pltpu.make_async_copy(pair_hbm.at[own_groups], own_pairs, first_sem.at[0]),
        pltpu.make_async_copy(weight_hbm, weight_ref, first_sem.at[1]),
        pltpu.make_async_copy(earlier_hbm, earlier_ref, first_sem.at[2]),
        pltpu.make_async_copy(gain_hbm, gain_ref, first_sem.at[3]),
    )
    for copy in first_copies:
        copy.start()
    pair_copy = pltpu.make_async_copy(pair_hbm, pair, local_sem.at[0])
    pair_copy.start()
    pieces = [pl.ds(c * chunk, chunk) for c in range(chunks)]
    x_copies = [pltpu.make_async_copy(x_hbm.at[:, :, cols], arriving.at[ahead[0], c], local_sem.at[1 + c])
                for c, cols in enumerate(pieces)]
    ct_copies = [pltpu.make_async_copy(ct_hbm.at[:, :, cols], arriving.at[ahead[1], c], local_sem.at[1 + c])
                 for c, cols in enumerate(pieces)]
    x_mates = [remote(x_hbm.at[:, :, cols], arriving.at[ahead[1], c], in_send.at[c], in_recv.at[c], mate)
               for c, cols in enumerate(pieces)]
    ct_mates = [remote(ct_hbm.at[:, :, cols], arriving.at[ahead[0], c], in_send.at[c], in_recv.at[c], mate)
                for c, cols in enumerate(pieces)]

    tail_mates = [remote(ct_hbm.at[pl.ds(micros // 2 - TAIL, TAIL), :, cols], hidden.at[pl.ds(early, TAIL), c],
                         in_send.at[c], in_recv.at[c], mate) for c, cols in enumerate(pieces)]

    @pl.when((s == 0) & forward_core)
    def _():
        for copy in x_copies:
            copy.start()

    @pl.when((s == last) & backward_core)
    def _():
        for copy in ct_copies:
            copy.start()

    barrier = pltpu.get_barrier_semaphore()
    for target in (*around, mate):
        pl.semaphore_signal(barrier, inc=1, device_id={"dp": target}, device_id_type=MESH)

    @pl.when(s > 0)
    def _():
        pl.semaphore_signal(barrier, inc=1, device_id={"section": s - 1}, device_id_type=MESH)

    @pl.when(s < last)
    def _():
        pl.semaphore_signal(barrier, inc=1, device_id={"section": s + 1}, device_id_type=MESH)

    piece = 128
    for copy in first_copies:
        copy.wait()
    counted = jnp.zeros((8, 128), jnp.int32)
    for k in range(width // piece):
        cols = pl.ds(k * piece, piece)
        p = own_pairs[:, cols]
        wide_rows[k] = weight_ref[:, cols].astype(F32)
        w0, w1, w2, w3 = (wide_rows[k, pl.ds(j, groups, stride=4), :] for j in range(4))
        lead = jnp.where(p < 3, w0, jnp.where(p == 5, w2, w1))
        trail = jnp.where(p == 0, w1, jnp.where((p == 1) | (p == 3), w2, w3))
        packed[dp, 0:groups, cols] = lead.astype(BF)
        packed[dp, groups:2 * groups, cols] = trail.astype(BF)
        kept = (p < 3, (p == 0) | (p == 3) | (p == 4), (p == 1) | (p == 3) | (p == 5), (p == 2) | (p > 3))
        for j, (k_j, w_j) in enumerate(zip(kept, (w0, w1, w2, w3))):
            decay[k, pl.ds(j, groups, stride=4), :] = jnp.where(k_j, 0.0, decay_rate * w_j)
        e = earlier_ref[:, cols]
        changed = jnp.where(p == e, 0, jnp.where(p + e == 5, 4, 2))
        for a in range(groups // 8):
            for b in range(piece // 128):
                counted = counted + changed[8 * a:8 * a + 8, 128 * b:128 * b + 128]
    flips[0] = counted

    pl.semaphore_wait(barrier, 5 + jnp.where(s > 0, 1, 0) + jnp.where(s < last, 1, 0))

    @pl.when((s == 0) & backward_core)
    def _():
        for copy in x_mates:
            copy.start()

    @pl.when((s == last) & forward_core)
    def _():
        for copy in ct_mates:
            copy.start()

    @pl.when((s == last) & backward_core)
    def _():
        for copy in tail_mates:
            copy.start()

    def shard_copy(b, d, recv):
        ref = packed.at[2 * b + core]
        return remote(ref, ref, ag_send.at[d], recv, (*around, mate)[d])

    def send_shard(b, d):
        shard_copy(b, d, ag_recv.at[b]).start()

    def wait_shard(b):
        shard_copy(b, 0, ag_recv.at[b]).wait_recv()

    def half_shard(b, h):
        ref = packed.at[2 * b + core, pl.ds(h * groups, groups)]
        return remote(ref, ref, ag_send.at[h], far_recv.at[h], around[h])

    def send_mate(b):
        shard_copy(b, 4, mate_recv.at[b]).start()

    def wait_mate(b):
        slot = 2 * b + (1 - core)
        remote(packed.at[slot], packed.at[slot], ag_send.at[4], mate_recv.at[b], mate).wait_recv()

    def spread(b):
        send_shard(b, 2)
        send_shard(b, 3)
        send_mate(b)

    def unpack(slot):
        at = pl.ds(pl.multiple_of(slot * groups, groups), groups)
        to = pl.ds(pl.multiple_of(slot * shard, shard), shard)
        for k in range(width // piece):
            cols = pl.ds(k * piece, piece)
            p = pair[at, cols]
            lead = packed[slot, 0:groups, cols].astype(F32)
            trail = packed[slot, groups:2 * groups, cols].astype(F32)
            o0 = jnp.where(p < 3, lead, 0.0)
            o1 = jnp.where(p == 0, trail, jnp.where((p == 3) | (p == 4), lead, 0.0))
            o2 = jnp.where(p == 5, lead, jnp.where((p == 1) | (p == 3), trail, 0.0))
            o3 = jnp.where((p == 2) | (p > 3), trail, 0.0)
            for j, o in enumerate((o0, o1, o2, o3)):
                wide_rows[k, pl.ds(j, groups, stride=4), :] = o
            w[to, cols] = wide_rows[k].astype(BF)

    def flip_copy(src, dst, target):
        return remote(flips.at[src], flips.at[dst], flip_send.at[dst - 1], flip_recv.at[dst - 1], target)

    own = chip(core, 0, 0)
    send_shard(own, 0)
    send_shard(own, 1)
    spread(own)
    flip_copy(0, 1, mate).start()
    pair_copy.wait()
    unpack(dp)
    from_left, from_right, far = chip(core, 3, 0), chip(core, 1, 0), chip(core, 2, 0)
    wait_shard(from_left)
    half_shard(from_left, 0).start()
    spread(from_left)
    wait_shard(from_right)
    half_shard(from_right, 1).start()
    spread(from_right)
    flip_copy(0, 1, mate).wait_recv()
    flips[8] = flips[0] + flips[1]
    flip_copy(8, 2, right1).start()
    flip_copy(8, 3, left1).start()
    unpack(2 * from_left + core)
    half_shard(far, 0).wait_recv()
    half_shard(far, 1).wait_recv()
    spread(far)

    def near(i, carry):
        r1 = jnp.where(i == 0, 0, jnp.where(i == 1, 3, jnp.where(i == 2, 1, 2)))
        lower, upper = chip(core, r1, 3), chip(core, r1, 1)
        wait_shard(lower)

        @pl.when(i < 2)
        def _():
            send_shard(lower, 2)

        send_mate(lower)
        wait_shard(upper)

        @pl.when(i >= 2)
        def _():
            send_shard(upper, 3)

        send_mate(upper)
        other = chip(1 - core, r1, 0)
        wait_mate(other)

        def expand(j, c):
            unpack(jnp.where(j == 0, 2 * other + (1 - core), jnp.where(j == 1, 2 * lower + core, 2 * upper + core)))
            return c

        lax.fori_loop(0, 3, expand, 0)
        return carry

    lax.fori_loop(0, SIDE, near, 0)

    def expand_rest(j, c):
        unpack(2 * jnp.where(j == 0, from_right, far) + core)
        return c

    lax.fori_loop(0, 2, expand_rest, 0)
    flip_copy(8, 2, right1).wait_recv()
    flip_copy(2, 4, right1).start()

    def distant(i, carry):
        r1 = jnp.where(i == 0, 0, jnp.where(i == 1, 3, jnp.where(i == 2, 1, 2)))
        beyond = chip(core, r1, 2)
        wait_shard(beyond)
        send_mate(beyond)
        lower, upper = chip(1 - core, r1, 3), chip(1 - core, r1, 1)
        wait_mate(lower)
        wait_mate(upper)

        def expand(j, c):
            unpack(jnp.where(j == 0, 2 * beyond + core,
                             jnp.where(j == 1, 2 * lower + (1 - core), 2 * upper + (1 - core))))
            return c

        lax.fori_loop(0, 3, expand, 0)
        return carry

    lax.fori_loop(0, SIDE, distant, 0)

    def final(i, carry):
        r1 = jnp.where(i == 0, 0, jnp.where(i == 1, 3, jnp.where(i == 2, 1, 2)))
        b = chip(1 - core, r1, 2)
        wait_mate(b)
        unpack(2 * b + (1 - core))
        return carry

    lax.fori_loop(0, SIDE, final, 0)

    flip_copy(8, 3, left1).wait_recv()
    flip_copy(2, 4, right1).wait_recv()
    flips[9] = flips[8] + flips[2] + flips[3] + flips[4]
    flip_copy(9, 5, right2).start()
    flip_copy(9, 6, left2).start()

    def tile_rows(m):
        return pl.ds(pl.multiple_of(m * rows, rows), rows)

    def z_copy(src, dst, send, recv, target):
        return pltpu.make_async_remote_copy(
            src_ref=src, dst_ref=dst, send_sem=send, recv_sem=recv, device_id={"section": target}, device_id_type=MESH)

    def forward_copy(m, *where):
        at = (m, *where)
        return z_copy(leaving.at[at], arriving.at[at], z_send.at[m], z_recv.at[m], jnp.minimum(s + 1, last))

    def backward_copy(m, *where):
        at = (m, *where)
        return z_copy(leaving.at[at], arriving.at[at], z_send.at[m], z_recv.at[m], jnp.maximum(s - 1, 0))

    def tail_copy(m, *where):
        return z_copy(tail_out.at[(m - early, *where)], hidden.at[(m, *where)], t_send.at[m - early],
                      t_recv.at[m - early], jnp.maximum(s - 1, 0))

    def half_copy(m):
        return remote(theirs.at[tile_rows(m)], mine.at[tile_rows(m)], mate_send.at[0, m], mate_n.at[m], mate)

    def grad_copy(m):
        return remote(grad_pre.at[tile_rows(m)], grad_pre.at[tile_rows(m)], mate_send.at[5, m], mate_g.at[m], mate)

    def saved_copy(k, m):
        src = (arriving, slope, preact, scale)[k]
        dst = (hidden, slope, preact, scale)[k]
        at = m if k == 0 else tile_rows(m)
        return remote(src.at[at], dst.at[at], mate_send.at[1 + k, m], mate_f.at[k, m], mate)

    def forward(m, carry):
        at = tile_rows(m)

        @pl.when(s > 0)
        def _():
            forward_copy(m).wait_recv()

        gained, squares = [], 0.0
        for c, cols in enumerate(pieces):
            values = arriving[m, c].astype(F32)
            gained.append((values * gain_ref[:, cols]).astype(BF))
            squares += jnp.sum(values * values, axis=-1, keepdims=True)
        gained = jnp.concatenate(gained, axis=1)
        q = lax.rsqrt(squares * (1.0 / width) + epsilon)
        scale[at, :] = jnp.broadcast_to(q, (rows, 128))
        for c, cols in enumerate(pieces):
            p = jnp.dot(gained, w[:, cols], preferred_element_type=F32) * q
            cdf = 0.5 * (1.0 + lax.erf(p * half_root))
            leaving[m, c] = (arriving[m, c].astype(F32) + p * cdf).astype(BF)

            @pl.when(s < last)
            def _():
                forward_copy(m, c).start()

            preact[at, cols] = p.astype(BF)
            slope[at, cols] = (cdf + p * (jnp.exp(-0.5 * p * p) * density_scale)).astype(BF)

        @pl.when(m < early)
        def _():
            for k in (1, 2, 0, 3):
                saved_copy(k, m).start()

        return carry

    def halves(m, carry):
        at = tile_rows(m)
        q = scale[at, :]
        low = lax.broadcasted_iota(jnp.int32, (rows, 128), 1) < 64

        def scaled(start):
            values = arriving[m, start // chunk, :, pl.ds(start % chunk, 128)].astype(F32)
            return values * q * gain_ref[:, pl.ds(start, 128)]

        for k in range(width // 256):
            first, second = scaled(256 * k), scaled(256 * k + 128)
            cols = pl.ds(128 * k, 128)
            mine[at, cols] = jnp.where(low, pltpu.roll(first, 64, 1), second).astype(BF)
        for k in range(width // 256):
            start = (k % 2) * 1024 + (k // 2) * 128
            first, second = scaled(start), scaled(start + 512)
            theirs[at, pl.ds(128 * k, 128)] = jnp.where(low, first, pltpu.roll(second, 64, 1)).astype(BF)
        half_copy(m).start()
        return carry

    def backward_rows(m, upstream, inputs, result, place, z):
        at = tile_rows(m)

        @pl.when(s < last)
        def _():
            z(m).wait_recv()

        gp = jnp.concatenate(
            [(upstream[m, c].astype(F32) * slope[at, cols].astype(F32)).astype(BF) for c, cols in enumerate(pieces)],
            axis=1)
        grad_pre[at, :] = gp

        @pl.when(s > 0)
        def _():
            q = scale[at, 0:1]
            mean = jnp.sum(gp.astype(F32) * preact[at, :].astype(F32), axis=-1, keepdims=True) * (1.0 / width)
            pull = q * q * mean
            for c, cols in enumerate(pieces):
                a = jnp.dot(gp, turned[:, cols], preferred_element_type=F32)
                a = a * gain_ref[:, cols]
                result[place, c] = (upstream[m, c].astype(F32) + q * a - inputs[m, c].astype(F32) * pull).astype(BF)
                z(m, c).start()

        grad_copy(m).start()

    def backward(m, carry):
        for k in (0, 1, 2, 3):
            saved_copy(k, m).wait_recv()
        backward_rows(m, arriving, hidden, leaving, m, backward_copy)
        return carry

    def backward_tail(m, carry):
        backward_rows(m, hidden, arriving, tail_out, m - early, tail_copy)
        return carry

    def turn(i, carry):
        at = pl.ds(pl.multiple_of(i * 128, 128), 128)
        turned[:, at] = w[at, :].T
        return carry

    def received_grad(m, carry):
        grad_copy(m).wait_recv()
        return carry

    def received_half(m, carry):
        half_copy(m).wait_recv()
        return carry

    @pl.when(forward_core)
    def _():
        @pl.when(s == 0)
        def _():
            for copy in x_copies:
                copy.wait()
            for copy in x_mates:
                copy.wait_recv()

        @pl.when(s > 1)
        def _():
            lax.fori_loop(0, width // 128, turn, 0)

        lax.fori_loop(0, micros, forward, 0)

        @pl.when(s == 1)
        def _():
            lax.fori_loop(0, width // 128, turn, 0)

        @pl.when(s < 4)
        def _():
            lax.fori_loop(0, micros, halves, 0)

        @pl.when(s == last)
        def _():
            for copy in tail_mates:
                copy.wait_recv()

        lax.fori_loop(early, micros, backward_tail, 0)

        @pl.when(s >= 4)
        def _():
            lax.fori_loop(0, micros, halves, 0)

        lax.fori_loop(0, early, received_grad, 0)

    @pl.when(backward_core)
    def _():
        lax.fori_loop(0, width // 128, turn, 0)

        @pl.when(s == last)
        def _():
            for copy in ct_copies:
                copy.wait()
            for copy in ct_mates:
                copy.wait_recv()

        lax.fori_loop(0, early, backward, 0)
        lax.fori_loop(0, micros, received_half, 0)
        lax.fori_loop(early, micros, received_grad, 0)

    flip_copy(9, 5, right2).wait_recv()
    flip_copy(5, 7, right2).start()

    place1, place2 = jnp.where(core == 0, xx, yy), jnp.where(core == 0, yy, xx)

    def block(r1, r2):
        place = ((place1 + r1) % SIDE) * SIDE + (place2 + r2) % SIDE
        return pl.ds(pl.multiple_of(place * shard, shard), shard)

    def terms(i):
        r1 = jnp.where(i == 0, 2, jnp.where(i == 1, 3, jnp.where(i == 2, 1, 0)))
        cols = pl.ds(pl.multiple_of(((place1 + r1) % SIDE) * (SIDE * shard), SIDE * shard), SIDE * shard)
        part[cols, :] = lax.dot_general(
            mine[:, cols], grad_pre[...], (((0,), (0,)), ((), ())), preferred_element_type=F32).astype(BF)

    def slot(r2, count=1):
        return pl.ds(r2 * shard, count * shard)

    def first_ring(src_r1, r2, d, dst, dst_slot, recv):
        return remote(part.at[block(src_r1, r2)], dst.at[dst_slot], rs_send.at[d], recv, around[d])

    toward_left, toward_right = (2, 1), (3, 0)
    def group(i, carry):
        terms(i)

        @pl.when(i == 0)
        def _():
            for k in range(2):
                first_ring(2, toward_left[k], 1, part_a, slot(toward_left[k]), a_recv.at[toward_left[k]]).start()
                first_ring(2, toward_right[k], 0, part_a, slot(toward_right[k]), a_recv.at[toward_right[k]]).start()

        @pl.when(i == 1)
        def _():
            for r2 in toward_right:
                first_ring(3, r2, 1, part_b, slot(r2), ab_recv.at[0, r2]).start()

        @pl.when(i == 2)
        def _():
            for r2 in toward_left:
                first_ring(1, r2, 0, part_b, slot(4 + r2), ab_recv.at[1, r2]).start()

        return carry

    lax.fori_loop(0, SIDE, group, 0)
    for k in range(2):
        for r2, r1, d, side in ((toward_left[k], 3, 1, 0), (toward_right[k], 1, 0, 1)):
            first_ring(2, r2, d, part_a, slot(r2), a_recv.at[r2]).wait_recv()
            at = block(r1, r2)
            part[at, :] = (part[at, :].astype(F32) + part_a[slot(r2), :].astype(F32)).astype(BF)
            first_ring(r1, r2, d, part_b, slot(4 * side + r2), ab_recv.at[side, r2]).start()

    flip_copy(9, 6, left2).wait_recv()
    flip_copy(5, 7, right2).wait_recv()
    all_flips = flips[9] + flips[5] + flips[6] + flips[7]
    flip_ref[0] = jnp.sum(all_flips.astype(F32)).astype(jnp.int32)

    def ring_total(r2):
        for side in range(2):
            first_ring(3, r2, 1, part_b, slot(4 * side + r2), ab_recv.at[side, r2]).wait_recv()
        total = part[block(0, r2), :].astype(F32) + part_b[slot(r2), :].astype(F32) + part_b[slot(4 + r2), :].astype(F32)
        row_sum[slot(r2), :] = total.astype(BF)

    half = shard // 2

    def second_ring(r2, h, d, dst, start, recv):
        return remote(row_sum.at[pl.ds(r2 * shard + h * half, half)], dst.at[pl.ds(start, half)], rs_send.at[d], recv,
                      around[d])

    ring_total(2)
    second_ring(2, 0, 3, row_a, 0, ra_recv.at[0]).start()
    second_ring(2, 1, 2, row_a, half, ra_recv.at[1]).start()
    ring_total(3)
    second_ring(3, 1, 3, row_b, half, rb_recv.at[0, 1]).start()
    ring_total(1)
    second_ring(1, 0, 2, row_b, shard, rb_recv.at[1, 0]).start()
    for h, r2, d, side in ((0, 3, 3, 0), (1, 1, 2, 1)):
        second_ring(2, h, d, row_a, h * half, ra_recv.at[h]).wait_recv()
        at = pl.ds(r2 * shard + h * half, half)
        row_sum[at, :] = (row_sum[at, :].astype(F32) + row_a[pl.ds(h * half, half), :].astype(F32)).astype(BF)
        second_ring(r2, h, d, row_b, side * shard + h * half, rb_recv.at[side, h]).start()
    ring_total(0)
    for side, h in ((0, 1), (1, 0), (0, 0), (1, 1)):
        second_ring(2, h, 3, row_b, side * shard + h * half, rb_recv.at[side, h]).wait_recv()
    for k in range(width // piece):
        cols = pl.ds(k * piece, piece)
        total = row_sum[slot(0), cols].astype(F32) + row_b[slot(0), cols].astype(F32) + row_b[slot(1), cols].astype(F32)
        out_ref[:, cols] = total * (1.0 / math.sqrt(token_total)) + decay[k]

    def drain_forward(m, carry):
        @pl.when(s < last)
        def _():
            forward_copy(m).wait_send()

        half_copy(m).wait_send()
        return carry

    def drain_saved(m, carry):
        for k in range(4):
            saved_copy(k, m).wait_send()
        return carry

    def drain_tail(m, carry):
        @pl.when(s > 0)
        def _():
            tail_copy(m).wait_send()

        grad_copy(m).wait_send()
        return carry

    def drain_backward(m, carry):
        @pl.when(s > 0)
        def _():
            backward_copy(m).wait_send()

        grad_copy(m).wait_send()
        return carry

    @pl.when(forward_core)
    def _():
        lax.fori_loop(0, micros, drain_forward, 0)
        lax.fori_loop(0, early, drain_saved, 0)
        lax.fori_loop(early, micros, drain_tail, 0)

        @pl.when(s == last)
        def _():
            for copy in ct_mates:
                copy.wait_send()

    @pl.when(backward_core)
    def _():
        lax.fori_loop(0, early, drain_backward, 0)

        @pl.when(s == last)
        def _():
            for copy in tail_mates:
                copy.wait_send()

        @pl.when(s == 0)
        def _():
            for copy in x_mates:
                copy.wait_send()

    def sent(sem, count):
        ref = grad_pre.at[pl.ds(0, count)]
        remote(ref, ref, sem, flip_recv.at[0], mate).wait_send()

    for d in (0, 1):
        sent(ag_send.at[d], 3 * groups)
    for d in (2, 3):
        sent(ag_send.at[d], 12 * groups)
    sent(ag_send.at[4], 2 * BLOCKS * groups)
    for d in (0, 1):
        sent(rs_send.at[d], 6 * shard)
    for d in (2, 3):
        sent(rs_send.at[d], 3 * half)
    for dst in range(1, 8):
        flip_copy(0, dst, mate).wait_send()


def step(x, ct, weight, gain, pair, earlier, sections, token_total, chunk):
    micros, tall, width = x.shape
    micros, rows = 2 * micros, micros * tall
    chunks = width // chunk
    shard = weight.shape[0]
    groups = shard // 4
    vmem = pl.BlockSpec(memory_space=pltpu.VMEM)
    hbm = pl.BlockSpec(memory_space=pl.ANY)
    act = pltpu.VMEM((2 * rows, width), BF)
    stream = pltpu.VMEM((micros, chunks, tall, chunk), BF)
    dma = pltpu.SemaphoreType.DMA
    return pl.pallas_call(
        functools.partial(kernel, sections, token_total),
        out_shape=(jax.ShapeDtypeStruct((shard, width), F32), jax.ShapeDtypeStruct((1,), jnp.int32)),
        in_specs=[hbm] * 6,
        out_specs=(vmem, pl.BlockSpec(memory_space=pltpu.SMEM)),
        scratch_shapes=[
            pltpu.VMEM((shard, width), BF), pltpu.VMEM((1, width), F32), pltpu.VMEM((groups, width), jnp.int32),
            pltpu.VMEM((groups, width), jnp.int32), dma((4,)),
            pltpu.VMEM((width, width), BF),
            pltpu.VMEM((width, width), BF),
            pltpu.VMEM((2 * BLOCKS, 2 * groups, width), BF),
            pltpu.VMEM(pair.shape, jnp.int32),
            pltpu.VMEM((width // 128, shard, 128), F32),
            pltpu.VMEM((width // 128, shard, 128), F32),
            stream, stream, stream, pltpu.VMEM((TAIL, chunks, tall, chunk), BF), dma((TAIL,)), dma((TAIL,)), act, act, pltpu.VMEM((2 * rows, 128), F32),
            pltpu.VMEM((2 * rows, width // 2), BF),
            pltpu.VMEM((2 * rows, width // 2), BF),
            pltpu.VMEM((2 * rows, width), BF),
            pltpu.VMEM((width // 2, width), BF),
            pltpu.VMEM((SIDE * shard, width), BF),
            pltpu.VMEM((2 * SIDE * shard, width), BF),
            pltpu.VMEM((SIDE * shard, width), BF),
            pltpu.VMEM((shard, width), BF),
            pltpu.VMEM((2 * shard, width), BF),
            pltpu.VMEM((10, 8, 128), jnp.int32),
            dma((1 + chunks,)), dma((5,)), dma((BLOCKS,)), dma((2,)), dma((BLOCKS,)), dma((chunks,)), dma((chunks,)),
            dma((micros,)), dma((micros,)), dma((micros,)), dma((micros,)), dma((4, micros)), dma((6, micros)),
            dma((SIDE,)), dma((2, SIDE)), dma((2,)), dma((2, 2)), dma((4,)), dma((7,)), dma((7,)),
        ],
        compiler_params=pltpu.CompilerParams(
            collective_id=0, has_side_effects=True, vmem_limit_bytes=58 * 1024 * 1024),
    )(x, ct, weight, gain, pair, earlier)


def body(activations, cotangent, weight, norm_gain, pair_mask, earlier_mask):
    micro_count, row_count, model_width = activations.shape
    tokens = micro_count * row_count
    tall = 32
    gradient, flip_sum = step(
        activations.reshape(tokens // tall, tall, model_width), cotangent.reshape(tokens // tall, tall, model_width),
        weight[0], norm_gain, pair_mask[0], earlier_mask[0], lax.axis_size("section"),
        tokens * lax.axis_size("dp"), CHUNK)
    return (gradient[None], flip_sum)


def solution(mesh):
    placed = (
        P(None, "dp", None),
        P(None, "dp", None),
        P("section", "dp", None),
        P("section", None),
        P("section", None, None),
        P("section", "dp", None),
    )
    return jax.shard_map(
        body,
        mesh=mesh,
        in_specs=placed,
        out_specs=(P("section", "dp", None), P("section")),
        check_vma=False,
    )
```

```python
import functools
import math

import jax
import jax.numpy as jnp
from jax import lax
from jax.experimental import pallas as pl
from jax.experimental.pallas import tpu as pltpu
from jax.sharding import PartitionSpec as P

MESH = pl.DeviceIdType.MESH
epsilon = 1e-06
decay_rate = 4.0
half_root = 0.7071067811865476
density_scale = 0.3989422804014327
BF = jnp.bfloat16
F32 = jnp.float32
SIDE = 4
CHUNK = 1024
BLOCKS = SIDE * SIDE


def kernel(sections, token_total, x_hbm, ct_hbm, weight_hbm, gain_hbm, pair_hbm, earlier_hbm, out_ref, flip_ref,
           weight_ref, gain_ref, earlier_ref, own_pairs, first_sem,
           partial, w, turned, packed, pair, wide_rows, decay, arriving, leaving, hidden, preact, slope, scale, mine, theirs,
           grad_pre, part, part_a, part_b, row_sum, row_a, row_b, flips,
           local_sem, ag_send, ag_recv, far_recv, mate_recv, in_send, in_recv, z_send, z_recv, mate_n, mate_g, mate_f, mate_send,
           a_recv, ab_recv, ra_recv, rb_recv, rs_send, flip_send, flip_recv):
    s = lax.axis_index("section")
    dp = lax.axis_index("dp")
    core, xx, yy = dp % 2, (dp // 2) % SIDE, dp // (2 * SIDE)
    last = sections - 1
    micros, chunks, rows, chunk = arriving.shape
    width = chunks * chunk
    ahead = pl.ds(0, micros // 2), pl.ds(micros // 2, micros // 2)
    forward_core, backward_core = core == 1, core == 0
    shard = weight_ref.shape[0]
    groups = shard // 4
    half_width = width // 2

    def chip(plane, r1, r2):
        dx, dy = jnp.where(plane == 0, r1, r2), jnp.where(plane == 0, r2, r1)
        return ((yy + dy) % SIDE) * SIDE + (xx + dx) % SIDE

    mate = 2 * (dp // 2) + (1 - core)
    right1, left1 = 2 * chip(core, 1, 0) + core, 2 * chip(core, 3, 0) + core
    right2, left2 = 2 * chip(core, 0, 1) + core, 2 * chip(core, 0, 3) + core
    around = (right1, left1, right2, left2)

    def remote(src, dst, send, recv, target):
        return pltpu.make_async_remote_copy(
            src_ref=src, dst_ref=dst, send_sem=send, recv_sem=recv, device_id={"dp": target}, device_id_type=MESH)

    own_groups = pl.ds(pl.multiple_of(dp * groups, groups), groups)
    first_copies = (
        pltpu.make_async_copy(pair_hbm.at[own_groups], own_pairs, first_sem.at[0]),
        pltpu.make_async_copy(weight_hbm, weight_ref, first_sem.at[1]),
        pltpu.make_async_copy(earlier_hbm, earlier_ref, first_sem.at[2]),
        pltpu.make_async_copy(gain_hbm, gain_ref, first_sem.at[3]),
    )
    for copy in first_copies:
        copy.start()
    pair_copy = pltpu.make_async_copy(pair_hbm, pair, local_sem.at[0])
    pair_copy.start()
    pieces = [pl.ds(c * chunk, chunk) for c in range(chunks)]
    x_copies = [pltpu.make_async_copy(x_hbm.at[:, :, cols], arriving.at[ahead[0], c], local_sem.at[1 + c])
                for c, cols in enumerate(pieces)]
    ct_copies = [pltpu.make_async_copy(ct_hbm.at[:, :, cols], arriving.at[ahead[1], c], local_sem.at[1 + c])
                 for c, cols in enumerate(pieces)]
    x_mates = [remote(x_hbm.at[:, :, cols], arriving.at[ahead[1], c], in_send.at[c], in_recv.at[c], mate)
               for c, cols in enumerate(pieces)]
    ct_mates = [remote(ct_hbm.at[:, :, cols], arriving.at[ahead[0], c], in_send.at[c], in_recv.at[c], mate)
                for c, cols in enumerate(pieces)]

    @pl.when((s == 0) & forward_core)
    def _():
        for copy in x_copies:
            copy.start()

    @pl.when((s == last) & backward_core)
    def _():
        for copy in ct_copies:
            copy.start()

    barrier = pltpu.get_barrier_semaphore()
    for target in (*around, mate):
        pl.semaphore_signal(barrier, inc=1, device_id={"dp": target}, device_id_type=MESH)

    @pl.when(s > 0)
    def _():
        pl.semaphore_signal(barrier, inc=1, device_id={"section": s - 1}, device_id_type=MESH)

    @pl.when(s < last)
    def _():
        pl.semaphore_signal(barrier, inc=1, device_id={"section": s + 1}, device_id_type=MESH)

    piece = 128
    for copy in first_copies:
        copy.wait()
    counted = jnp.zeros((8, 128), jnp.int32)
    for k in range(width // piece):
        cols = pl.ds(k * piece, piece)
        p = own_pairs[:, cols]
        wide_rows[k] = weight_ref[:, cols].astype(F32)
        w0, w1, w2, w3 = (wide_rows[k, pl.ds(j, groups, stride=4), :] for j in range(4))
        lead = jnp.where(p < 3, w0, jnp.where(p == 5, w2, w1))
        trail = jnp.where(p == 0, w1, jnp.where((p == 1) | (p == 3), w2, w3))
        packed[dp, 0:groups, cols] = lead.astype(BF)
        packed[dp, groups:2 * groups, cols] = trail.astype(BF)
        kept = (p < 3, (p == 0) | (p == 3) | (p == 4), (p == 1) | (p == 3) | (p == 5), (p == 2) | (p > 3))
        for j, (k_j, w_j) in enumerate(zip(kept, (w0, w1, w2, w3))):
            decay[k, pl.ds(j, groups, stride=4), :] = jnp.where(k_j, 0.0, decay_rate * w_j)
        e = earlier_ref[:, cols]
        changed = jnp.where(p == e, 0, jnp.where(p + e == 5, 4, 2))
        for a in range(groups // 8):
            for b in range(piece // 128):
                counted = counted + changed[8 * a:8 * a + 8, 128 * b:128 * b + 128]
    flips[0] = counted

    pl.semaphore_wait(barrier, 5 + jnp.where(s > 0, 1, 0) + jnp.where(s < last, 1, 0))

    @pl.when((s == 0) & backward_core)
    def _():
        for copy in x_mates:
            copy.start()

    @pl.when((s == last) & forward_core)
    def _():
        for copy in ct_mates:
            copy.start()

    def shard_copy(b, d, recv):
        ref = packed.at[2 * b + core]
        return remote(ref, ref, ag_send.at[d], recv, (*around, mate)[d])

    def send_shard(b, d):
        shard_copy(b, d, ag_recv.at[b]).start()

    def wait_shard(b):
        shard_copy(b, 0, ag_recv.at[b]).wait_recv()

    def half_shard(b, h):
        ref = packed.at[2 * b + core, pl.ds(h * groups, groups)]
        return remote(ref, ref, ag_send.at[h], far_recv.at[h], around[h])

    def send_mate(b):
        shard_copy(b, 4, mate_recv.at[b]).start()

    def wait_mate(b):
        slot = 2 * b + (1 - core)
        remote(packed.at[slot], packed.at[slot], ag_send.at[4], mate_recv.at[b], mate).wait_recv()

    def spread(b):
        send_shard(b, 2)
        send_shard(b, 3)
        send_mate(b)

    def unpack(slot):
        at = pl.ds(pl.multiple_of(slot * groups, groups), groups)
        to = pl.ds(pl.multiple_of(slot * shard, shard), shard)
        for k in range(width // piece):
            cols = pl.ds(k * piece, piece)
            p = pair[at, cols]
            lead = packed[slot, 0:groups, cols].astype(F32)
            trail = packed[slot, groups:2 * groups, cols].astype(F32)
            o0 = jnp.where(p < 3, lead, 0.0)
            o1 = jnp.where(p == 0, trail, jnp.where((p == 3) | (p == 4), lead, 0.0))
            o2 = jnp.where(p == 5, lead, jnp.where((p == 1) | (p == 3), trail, 0.0))
            o3 = jnp.where((p == 2) | (p > 3), trail, 0.0)
            for j, o in enumerate((o0, o1, o2, o3)):
                wide_rows[k, pl.ds(j, groups, stride=4), :] = o
            w[to, cols] = wide_rows[k].astype(BF)

    def flip_copy(src, dst, target):
        return remote(flips.at[src], flips.at[dst], flip_send.at[dst - 1], flip_recv.at[dst - 1], target)

    own = chip(core, 0, 0)
    send_shard(own, 0)
    send_shard(own, 1)
    spread(own)
    flip_copy(0, 1, mate).start()
    pair_copy.wait()
    unpack(dp)
    from_left, from_right, far = chip(core, 3, 0), chip(core, 1, 0), chip(core, 2, 0)
    wait_shard(from_left)
    half_shard(from_left, 0).start()
    spread(from_left)
    wait_shard(from_right)
    half_shard(from_right, 1).start()
    spread(from_right)
    flip_copy(0, 1, mate).wait_recv()
    flips[8] = flips[0] + flips[1]
    flip_copy(8, 2, right1).start()
    flip_copy(8, 3, left1).start()
    unpack(2 * from_left + core)
    half_shard(far, 0).wait_recv()
    half_shard(far, 1).wait_recv()
    spread(far)

    def near(i, carry):
        r1 = jnp.where(i == 0, 0, jnp.where(i == 1, 3, jnp.where(i == 2, 1, 2)))
        lower, upper = chip(core, r1, 3), chip(core, r1, 1)
        wait_shard(lower)

        @pl.when(i < 2)
        def _():
            send_shard(lower, 2)

        send_mate(lower)
        wait_shard(upper)

        @pl.when(i >= 2)
        def _():
            send_shard(upper, 3)

        send_mate(upper)
        other = chip(1 - core, r1, 0)
        wait_mate(other)

        def expand(j, c):
            unpack(jnp.where(j == 0, 2 * other + (1 - core), jnp.where(j == 1, 2 * lower + core, 2 * upper + core)))
            return c

        lax.fori_loop(0, 3, expand, 0)
        return carry

    lax.fori_loop(0, SIDE, near, 0)

    def expand_rest(j, c):
        unpack(2 * jnp.where(j == 0, from_right, far) + core)
        return c

    lax.fori_loop(0, 2, expand_rest, 0)
    flip_copy(8, 2, right1).wait_recv()
    flip_copy(2, 4, right1).start()

    def distant(i, carry):
        r1 = jnp.where(i == 0, 0, jnp.where(i == 1, 3, jnp.where(i == 2, 1, 2)))
        beyond = chip(core, r1, 2)
        wait_shard(beyond)
        send_mate(beyond)
        lower, upper = chip(1 - core, r1, 3), chip(1 - core, r1, 1)
        wait_mate(lower)
        wait_mate(upper)

        def expand(j, c):
            unpack(jnp.where(j == 0, 2 * beyond + core,
                             jnp.where(j == 1, 2 * lower + (1 - core), 2 * upper + (1 - core))))
            return c

        lax.fori_loop(0, 3, expand, 0)
        return carry

    lax.fori_loop(0, SIDE, distant, 0)

    def final(i, carry):
        r1 = jnp.where(i == 0, 0, jnp.where(i == 1, 3, jnp.where(i == 2, 1, 2)))
        b = chip(1 - core, r1, 2)
        wait_mate(b)
        unpack(2 * b + (1 - core))
        return carry

    lax.fori_loop(0, SIDE, final, 0)

    flip_copy(8, 3, left1).wait_recv()
    flip_copy(2, 4, right1).wait_recv()
    flips[9] = flips[8] + flips[2] + flips[3] + flips[4]
    flip_copy(9, 5, right2).start()
    flip_copy(9, 6, left2).start()

    def tile_rows(m):
        return pl.ds(pl.multiple_of(m * rows, rows), rows)

    def z_copy(m, c, target):
        return pltpu.make_async_remote_copy(
            src_ref=leaving.at[m, c], dst_ref=arriving.at[m, c], send_sem=z_send.at[m, c], recv_sem=z_recv.at[m, c],
            device_id={"section": target}, device_id_type=MESH)

    def forward_copy(m, c):
        return z_copy(m, c, jnp.minimum(s + 1, last))

    def backward_copy(m, c):
        return z_copy(m, c, jnp.maximum(s - 1, 0))

    def half_copy(m):
        return remote(theirs.at[tile_rows(m)], mine.at[tile_rows(m)], mate_send.at[0, m], mate_n.at[m], mate)

    def grad_copy(m):
        return remote(grad_pre.at[tile_rows(m)], grad_pre.at[tile_rows(m)], mate_send.at[0, m], mate_g.at[m], mate)

    def saved_copy(k, m):
        src = (arriving, slope, preact, scale)[k]
        dst = (hidden, slope, preact, scale)[k]
        at = m if k == 0 else tile_rows(m)
        return remote(src.at[at], dst.at[at], mate_send.at[1 + k, m], mate_f.at[k, m], mate)

    def forward(m, carry):
        at = tile_rows(m)
        squares = 0.0
        for k, deep in enumerate(pieces):
            @pl.when(s > 0)
            def _():
                forward_copy(m, k).wait_recv()

            values = arriving[m, k].astype(F32)
            gained = (values * gain_ref[:, deep]).astype(BF)
            squares += jnp.sum(values * values, axis=-1, keepdims=True)
            if k < chunks - 1:
                for cols in pieces:
                    term = jnp.dot(gained, w[deep, cols], preferred_element_type=F32)
                    partial[:, cols] = term if k == 0 else partial[:, cols] + term
        q = lax.rsqrt(squares * (1.0 / width) + epsilon)
        scale[at, :] = jnp.broadcast_to(q, (rows, 128))
        for c, cols in enumerate(pieces):
            p = (partial[:, cols] + jnp.dot(gained, w[deep, cols], preferred_element_type=F32)) * q
            cdf = 0.5 * (1.0 + lax.erf(p * half_root))
            leaving[m, c] = (arriving[m, c].astype(F32) + p * cdf).astype(BF)

            @pl.when(s < last)
            def _():
                forward_copy(m, c).start()

            preact[at, cols] = p.astype(BF)
            slope[at, cols] = (cdf + p * (jnp.exp(-0.5 * p * p) * density_scale)).astype(BF)
        for k in (1, 2, 0, 3):
            saved_copy(k, m).start()
        return carry

    def halves(m, carry):
        at = tile_rows(m)
        q = scale[at, :]
        low = lax.broadcasted_iota(jnp.int32, (rows, 128), 1) < 64

        def scaled(start):
            values = arriving[m, start // chunk, :, pl.ds(start % chunk, 128)].astype(F32)
            return values * q * gain_ref[:, pl.ds(start, 128)]

        for k in range(width // 256):
            first, second = scaled(256 * k), scaled(256 * k + 128)
            cols = pl.ds(128 * k, 128)
            mine[at, cols] = jnp.where(low, pltpu.roll(first, 64, 1), second).astype(BF)
        for k in range(width // 256):
            start = (k % 2) * 1024 + (k // 2) * 128
            first, second = scaled(start), scaled(start + 512)
            theirs[at, pl.ds(128 * k, 128)] = jnp.where(low, first, pltpu.roll(second, 64, 1)).astype(BF)
        half_copy(m).start()
        return carry

    def backward(m, carry):
        at = tile_rows(m)
        for k in (0, 1, 2, 3):
            saved_copy(k, m).wait_recv()
        inner = 0.0
        for k, deep in enumerate(pieces):
            @pl.when(s < last)
            def _():
                backward_copy(m, k).wait_recv()

            gp = (arriving[m, k].astype(F32) * slope[at, deep].astype(F32)).astype(BF)
            grad_pre[at, deep] = gp
            inner += jnp.sum(gp.astype(F32) * preact[at, deep].astype(F32), axis=-1, keepdims=True)
            if k < chunks - 1:
                @pl.when(s > 0)
                def _():
                    for cols in pieces:
                        term = jnp.dot(gp, turned[deep, cols], preferred_element_type=F32)
                        partial[:, cols] = term if k == 0 else partial[:, cols] + term

        @pl.when(s > 0)
        def _():
            q = scale[at, 0:1]
            pull = q * q * (inner * (1.0 / width))
            for c, cols in enumerate(pieces):
                a = partial[:, cols] + jnp.dot(gp, turned[deep, cols], preferred_element_type=F32)
                a = a * gain_ref[:, cols]
                leaving[m, c] = (arriving[m, c].astype(F32) + q * a - hidden[m, c].astype(F32) * pull).astype(BF)
                backward_copy(m, c).start()

        grad_copy(m).start()
        return carry

    def received_grad(m, carry):
        grad_copy(m).wait_recv()
        return carry

    def received_half(m, carry):
        half_copy(m).wait_recv()
        return carry

    @pl.when(forward_core)
    def _():
        @pl.when(s == 0)
        def _():
            for copy in x_copies:
                copy.wait()
            for copy in x_mates:
                copy.wait_recv()

        lax.fori_loop(0, micros, forward, 0)
        lax.fori_loop(0, micros, halves, 0)
        lax.fori_loop(0, micros, received_grad, 0)

    @pl.when(backward_core)
    def _():
        def turn(i, carry):
            at = pl.ds(pl.multiple_of(i * 128, 128), 128)
            turned[:, at] = w[at, :].T
            return carry

        lax.fori_loop(0, width // 128, turn, 0)

        @pl.when(s == last)
        def _():
            for copy in ct_copies:
                copy.wait()
            for copy in ct_mates:
                copy.wait_recv()

        lax.fori_loop(0, micros, backward, 0)
        lax.fori_loop(0, micros, received_half, 0)

    flip_copy(9, 5, right2).wait_recv()
    flip_copy(5, 7, right2).start()

    place1, place2 = jnp.where(core == 0, xx, yy), jnp.where(core == 0, yy, xx)

    def block(r1, r2):
        place = ((place1 + r1) % SIDE) * SIDE + (place2 + r2) % SIDE
        return pl.ds(pl.multiple_of(place * shard, shard), shard)

    def terms(i):
        r1 = jnp.where(i == 0, 2, jnp.where(i == 1, 3, jnp.where(i == 2, 1, 0)))
        cols = pl.ds(pl.multiple_of(((place1 + r1) % SIDE) * (SIDE * shard), SIDE * shard), SIDE * shard)
        part[cols, :] = lax.dot_general(
            mine[:, cols], grad_pre[...], (((0,), (0,)), ((), ())), preferred_element_type=F32).astype(BF)

    def slot(r2, count=1):
        return pl.ds(r2 * shard, count * shard)

    def first_ring(src_r1, r2, d, dst, dst_slot, recv):
        return remote(part.at[block(src_r1, r2)], dst.at[dst_slot], rs_send.at[d], recv, around[d])

    toward_left, toward_right = (2, 1), (3, 0)
    def group(i, carry):
        terms(i)

        @pl.when(i == 0)
        def _():
            for k in range(2):
                first_ring(2, toward_left[k], 1, part_a, slot(toward_left[k]), a_recv.at[toward_left[k]]).start()
                first_ring(2, toward_right[k], 0, part_a, slot(toward_right[k]), a_recv.at[toward_right[k]]).start()

        @pl.when(i == 1)
        def _():
            for r2 in toward_right:
                first_ring(3, r2, 1, part_b, slot(r2), ab_recv.at[0, r2]).start()

        @pl.when(i == 2)
        def _():
            for r2 in toward_left:
                first_ring(1, r2, 0, part_b, slot(4 + r2), ab_recv.at[1, r2]).start()

        return carry

    lax.fori_loop(0, SIDE, group, 0)
    def drain_forward(m, carry):
        @pl.when(s < last)
        def _():
            for c in range(chunks):
                forward_copy(m, c).wait_send()

        half_copy(m).wait_send()
        for k in range(4):
            saved_copy(k, m).wait_send()
        return carry

    def drain_backward(m, carry):
        @pl.when(s > 0)
        def _():
            for c in range(chunks):
                backward_copy(m, c).wait_send()

        grad_copy(m).wait_send()
        return carry

    @pl.when(forward_core)
    def _():
        lax.fori_loop(0, micros, drain_forward, 0)

        @pl.when(s == last)
        def _():
            for copy in ct_mates:
                copy.wait_send()

    @pl.when(backward_core)
    def _():
        lax.fori_loop(0, micros, drain_backward, 0)

        @pl.when(s == 0)
        def _():
            for copy in x_mates:
                copy.wait_send()

    def sent(sem, count):
        ref = grad_pre.at[pl.ds(0, count)]
        remote(ref, ref, sem, flip_recv.at[0], mate).wait_send()

    for d in (0, 1):
        sent(ag_send.at[d], 3 * groups)
    for d in (2, 3):
        sent(ag_send.at[d], 12 * groups)
    sent(ag_send.at[4], 2 * BLOCKS * groups)

    for k in range(2):
        for r2, r1, d, side in ((toward_left[k], 3, 1, 0), (toward_right[k], 1, 0, 1)):
            first_ring(2, r2, d, part_a, slot(r2), a_recv.at[r2]).wait_recv()
            at = block(r1, r2)
            part[at, :] = (part[at, :].astype(F32) + part_a[slot(r2), :].astype(F32)).astype(BF)
            first_ring(r1, r2, d, part_b, slot(4 * side + r2), ab_recv.at[side, r2]).start()

    flip_copy(9, 6, left2).wait_recv()
    flip_copy(5, 7, right2).wait_recv()
    all_flips = flips[9] + flips[5] + flips[6] + flips[7]
    flip_ref[0] = jnp.sum(all_flips.astype(F32)).astype(jnp.int32)

    def ring_total(r2):
        for side in range(2):
            first_ring(3, r2, 1, part_b, slot(4 * side + r2), ab_recv.at[side, r2]).wait_recv()
        total = part[block(0, r2), :].astype(F32) + part_b[slot(r2), :].astype(F32) + part_b[slot(4 + r2), :].astype(F32)
        row_sum[slot(r2), :] = total.astype(BF)

    half = shard // 2

    def second_ring(r2, h, d, dst, start, recv):
        return remote(row_sum.at[pl.ds(r2 * shard + h * half, half)], dst.at[pl.ds(start, half)], rs_send.at[d], recv,
                      around[d])

    ring_total(2)
    second_ring(2, 0, 3, row_a, 0, ra_recv.at[0]).start()
    second_ring(2, 1, 2, row_a, half, ra_recv.at[1]).start()
    ring_total(3)
    second_ring(3, 1, 3, row_b, half, rb_recv.at[0, 1]).start()
    ring_total(1)
    second_ring(1, 0, 2, row_b, shard, rb_recv.at[1, 0]).start()
    for h, r2, d, side in ((0, 3, 3, 0), (1, 1, 2, 1)):
        second_ring(2, h, d, row_a, h * half, ra_recv.at[h]).wait_recv()
        at = pl.ds(r2 * shard + h * half, half)
        row_sum[at, :] = (row_sum[at, :].astype(F32) + row_a[pl.ds(h * half, half), :].astype(F32)).astype(BF)
        second_ring(r2, h, d, row_b, side * shard + h * half, rb_recv.at[side, h]).start()
    ring_total(0)
    for side, h in ((0, 1), (1, 0), (0, 0), (1, 1)):
        second_ring(2, h, 3, row_b, side * shard + h * half, rb_recv.at[side, h]).wait_recv()
    for k in range(width // piece):
        cols = pl.ds(k * piece, piece)
        total = row_sum[slot(0), cols].astype(F32) + row_b[slot(0), cols].astype(F32) + row_b[slot(1), cols].astype(F32)
        out_ref[:, cols] = total * (1.0 / math.sqrt(token_total)) + decay[k]

    for d in (0, 1):
        sent(rs_send.at[d], 6 * shard)
    for d in (2, 3):
        sent(rs_send.at[d], 3 * half)
    for dst in range(1, 8):
        flip_copy(0, dst, mate).wait_send()


def step(x, ct, weight, gain, pair, earlier, sections, token_total, chunk):
    micros, tall, width = x.shape
    micros, rows = 2 * micros, micros * tall
    chunks = width // chunk
    shard = weight.shape[0]
    groups = shard // 4
    vmem = pl.BlockSpec(memory_space=pltpu.VMEM)
    hbm = pl.BlockSpec(memory_space=pl.ANY)
    act = pltpu.VMEM((2 * rows, width), BF)
    stream = pltpu.VMEM((micros, chunks, tall, chunk), BF)
    dma = pltpu.SemaphoreType.DMA
    return pl.pallas_call(
        functools.partial(kernel, sections, token_total),
        out_shape=(jax.ShapeDtypeStruct((shard, width), F32), jax.ShapeDtypeStruct((1,), jnp.int32)),
        in_specs=[hbm] * 6,
        out_specs=(vmem, pl.BlockSpec(memory_space=pltpu.SMEM)),
        scratch_shapes=[
            pltpu.VMEM((shard, width), BF), pltpu.VMEM((1, width), F32), pltpu.VMEM((groups, width), jnp.int32),
            pltpu.VMEM((groups, width), jnp.int32), dma((4,)),
            pltpu.VMEM((tall, width), F32),
            pltpu.VMEM((width, width), BF),
            pltpu.VMEM((width, width), BF),
            pltpu.VMEM((2 * BLOCKS, 2 * groups, width), BF),
            pltpu.VMEM(pair.shape, jnp.int32),
            pltpu.VMEM((width // 128, shard, 128), F32),
            pltpu.VMEM((width // 128, shard, 128), F32),
            stream, stream, stream, act, act, pltpu.VMEM((2 * rows, 128), F32),
            pltpu.VMEM((2 * rows, width // 2), BF),
            pltpu.VMEM((2 * rows, width // 2), BF),
            pltpu.VMEM((2 * rows, width), BF),
            pltpu.VMEM((width // 2, width), BF),
            pltpu.VMEM((SIDE * shard, width), BF),
            pltpu.VMEM((2 * SIDE * shard, width), BF),
            pltpu.VMEM((SIDE * shard, width), BF),
            pltpu.VMEM((shard, width), BF),
            pltpu.VMEM((2 * shard, width), BF),
            pltpu.VMEM((10, 8, 128), jnp.int32),
            dma((1 + chunks,)), dma((5,)), dma((BLOCKS,)), dma((2,)), dma((BLOCKS,)), dma((chunks,)), dma((chunks,)),
            dma((micros, chunks)), dma((micros, chunks)), dma((micros,)), dma((micros,)), dma((4, micros)), dma((5, micros)),
            dma((SIDE,)), dma((2, SIDE)), dma((2,)), dma((2, 2)), dma((4,)), dma((7,)), dma((7,)),
        ],
        compiler_params=pltpu.CompilerParams(
            collective_id=0, has_side_effects=True, vmem_limit_bytes=58 * 1024 * 1024),
    )(x, ct, weight, gain, pair, earlier)


def body(activations, cotangent, weight, norm_gain, pair_mask, earlier_mask):
    micro_count, row_count, model_width = activations.shape
    tokens = micro_count * row_count
    tall = 32
    gradient, flip_sum = step(
        activations.reshape(tokens // tall, tall, model_width), cotangent.reshape(tokens // tall, tall, model_width),
        weight[0], norm_gain, pair_mask[0], earlier_mask[0], lax.axis_size("section"),
        tokens * lax.axis_size("dp"), CHUNK)
    return (gradient[None], flip_sum)


def solution(mesh):
    placed = (
        P(None, "dp", None),
        P(None, "dp", None),
        P("section", "dp", None),
        P("section", None),
        P("section", None, None),
        P("section", "dp", None),
    )
    return jax.shard_map(
        body,
        mesh=mesh,
        in_specs=placed,
        out_specs=(P("section", "dp", None), P("section")),
        check_vma=False,
    )
```

```python
import functools
import math

import jax
import jax.numpy as jnp
from jax import lax
from jax.experimental import pallas as pl
from jax.experimental.pallas import tpu as pltpu
from jax.sharding import PartitionSpec as P

MESH = pl.DeviceIdType.MESH
epsilon = 1e-06
decay_rate = 4.0
half_root = 0.7071067811865476
density_scale = 0.3989422804014327
BF = jnp.bfloat16
F32 = jnp.float32
SIDE = 4
CHUNK = 1024
BLOCKS = SIDE * SIDE


def kernel(sections, token_total, x_hbm, ct_hbm, weight_hbm, gain_hbm, pair_hbm, earlier_hbm, out_ref, flip_ref,
           weight_ref, gain_ref, earlier_ref, own_pairs, first_sem,
           partial, w, turned, packed, pair, wide_rows, decay, arriving, leaving, hidden, preact, slope, scale, mine, theirs,
           grad_pre, part, part_a, part_b, row_sum, row_a, row_b, flips,
           local_sem, ag_send, ag_recv, far_recv, mate_recv, in_send, in_recv, z_send, z_recv, mate_n, mate_g, mate_f, mate_send,
           a_recv, ab_recv, ra_recv, rb_recv, rs_send, flip_send, flip_recv):
    s = lax.axis_index("section")
    dp = lax.axis_index("dp")
    core, xx, yy = dp % 2, (dp // 2) % SIDE, dp // (2 * SIDE)
    last = sections - 1
    micros, chunks, rows, chunk = arriving.shape
    width = chunks * chunk
    ahead = pl.ds(0, micros // 2), pl.ds(micros // 2, micros // 2)
    forward_core, backward_core = core == 1, core == 0
    shard = weight_ref.shape[0]
    groups = shard // 4
    half_width = width // 2

    def chip(plane, r1, r2):
        dx, dy = jnp.where(plane == 0, r1, r2), jnp.where(plane == 0, r2, r1)
        return ((yy + dy) % SIDE) * SIDE + (xx + dx) % SIDE

    mate = 2 * (dp // 2) + (1 - core)
    right1, left1 = 2 * chip(core, 1, 0) + core, 2 * chip(core, 3, 0) + core
    right2, left2 = 2 * chip(core, 0, 1) + core, 2 * chip(core, 0, 3) + core
    around = (right1, left1, right2, left2)

    def remote(src, dst, send, recv, target):
        return pltpu.make_async_remote_copy(
            src_ref=src, dst_ref=dst, send_sem=send, recv_sem=recv, device_id={"dp": target}, device_id_type=MESH)

    own_groups = pl.ds(pl.multiple_of(dp * groups, groups), groups)
    first_copies = (
        pltpu.make_async_copy(pair_hbm.at[own_groups], own_pairs, first_sem.at[0]),
        pltpu.make_async_copy(weight_hbm, weight_ref, first_sem.at[1]),
        pltpu.make_async_copy(earlier_hbm, earlier_ref, first_sem.at[2]),
        pltpu.make_async_copy(gain_hbm, gain_ref, first_sem.at[3]),
    )
    for copy in first_copies:
        copy.start()
    pair_copy = pltpu.make_async_copy(pair_hbm, pair, local_sem.at[0])
    pair_copy.start()
    pieces = [pl.ds(c * chunk, chunk) for c in range(chunks)]
    x_copies = [pltpu.make_async_copy(x_hbm.at[:, :, cols], arriving.at[ahead[0], c], local_sem.at[1 + c])
                for c, cols in enumerate(pieces)]
    ct_copies = [pltpu.make_async_copy(ct_hbm.at[:, :, cols], arriving.at[ahead[1], c], local_sem.at[1 + c])
                 for c, cols in enumerate(pieces)]
    x_mates = [remote(x_hbm.at[:, :, cols], arriving.at[ahead[1], c], in_send.at[c], in_recv.at[c], mate)
               for c, cols in enumerate(pieces)]
    ct_mates = [remote(ct_hbm.at[:, :, cols], arriving.at[ahead[0], c], in_send.at[c], in_recv.at[c], mate)
                for c, cols in enumerate(pieces)]

    @pl.when((s == 0) & forward_core)
    def _():
        for copy in x_copies:
            copy.start()

    @pl.when((s == last) & backward_core)
    def _():
        for copy in ct_copies:
            copy.start()

    barrier = pltpu.get_barrier_semaphore()
    for target in (*around, mate):
        pl.semaphore_signal(barrier, inc=1, device_id={"dp": target}, device_id_type=MESH)

    @pl.when(s > 0)
    def _():
        pl.semaphore_signal(barrier, inc=1, device_id={"section": s - 1}, device_id_type=MESH)

    @pl.when(s < last)
    def _():
        pl.semaphore_signal(barrier, inc=1, device_id={"section": s + 1}, device_id_type=MESH)

    piece = 128
    for copy in first_copies:
        copy.wait()
    counted = jnp.zeros((8, 128), jnp.int32)
    for k in range(width // piece):
        cols = pl.ds(k * piece, piece)
        p = own_pairs[:, cols]
        wide_rows[k] = weight_ref[:, cols].astype(F32)
        w0, w1, w2, w3 = (wide_rows[k, pl.ds(j, groups, stride=4), :] for j in range(4))
        lead = jnp.where(p < 3, w0, jnp.where(p == 5, w2, w1))
        trail = jnp.where(p == 0, w1, jnp.where((p == 1) | (p == 3), w2, w3))
        packed[dp, 0:groups, cols] = lead.astype(BF)
        packed[dp, groups:2 * groups, cols] = trail.astype(BF)
        kept = (p < 3, (p == 0) | (p == 3) | (p == 4), (p == 1) | (p == 3) | (p == 5), (p == 2) | (p > 3))
        for j, (k_j, w_j) in enumerate(zip(kept, (w0, w1, w2, w3))):
            decay[k, pl.ds(j, groups, stride=4), :] = jnp.where(k_j, 0.0, decay_rate * w_j)
        e = earlier_ref[:, cols]
        changed = jnp.where(p == e, 0, jnp.where(p + e == 5, 4, 2))
        for a in range(groups // 8):
            for b in range(piece // 128):
                counted = counted + changed[8 * a:8 * a + 8, 128 * b:128 * b + 128]
    flips[0] = counted

    pl.semaphore_wait(barrier, 5 + jnp.where(s > 0, 1, 0) + jnp.where(s < last, 1, 0))

    @pl.when((s == 0) & backward_core)
    def _():
        for copy in x_mates:
            copy.start()

    @pl.when((s == last) & forward_core)
    def _():
        for copy in ct_mates:
            copy.start()

    def shard_copy(b, d, recv):
        ref = packed.at[2 * b + core]
        return remote(ref, ref, ag_send.at[d], recv, (*around, mate)[d])

    def send_shard(b, d):
        shard_copy(b, d, ag_recv.at[b]).start()

    def wait_shard(b):
        shard_copy(b, 0, ag_recv.at[b]).wait_recv()

    def half_shard(b, h):
        ref = packed.at[2 * b + core, pl.ds(h * groups, groups)]
        return remote(ref, ref, ag_send.at[h], far_recv.at[h], around[h])

    def send_mate(b):
        shard_copy(b, 4, mate_recv.at[b]).start()

    def wait_mate(b):
        slot = 2 * b + (1 - core)
        remote(packed.at[slot], packed.at[slot], ag_send.at[4], mate_recv.at[b], mate).wait_recv()

    def spread(b):
        send_shard(b, 2)
        send_shard(b, 3)
        send_mate(b)

    def unpack(slot):
        at = pl.ds(pl.multiple_of(slot * groups, groups), groups)
        to = pl.ds(pl.multiple_of(slot * shard, shard), shard)
        for k in range(width // piece):
            cols = pl.ds(k * piece, piece)
            p = pair[at, cols]
            lead = packed[slot, 0:groups, cols].astype(F32)
            trail = packed[slot, groups:2 * groups, cols].astype(F32)
            o0 = jnp.where(p < 3, lead, 0.0)
            o1 = jnp.where(p == 0, trail, jnp.where((p == 3) | (p == 4), lead, 0.0))
            o2 = jnp.where(p == 5, lead, jnp.where((p == 1) | (p == 3), trail, 0.0))
            o3 = jnp.where((p == 2) | (p > 3), trail, 0.0)
            for j, o in enumerate((o0, o1, o2, o3)):
                wide_rows[k, pl.ds(j, groups, stride=4), :] = o
            w[to, cols] = wide_rows[k].astype(BF)

    def flip_copy(src, dst, target):
        return remote(flips.at[src], flips.at[dst], flip_send.at[dst - 1], flip_recv.at[dst - 1], target)

    own = chip(core, 0, 0)
    send_shard(own, 0)
    send_shard(own, 1)
    spread(own)
    flip_copy(0, 1, mate).start()
    pair_copy.wait()
    unpack(dp)
    from_left, from_right, far = chip(core, 3, 0), chip(core, 1, 0), chip(core, 2, 0)
    wait_shard(from_left)
    half_shard(from_left, 0).start()
    spread(from_left)
    wait_shard(from_right)
    half_shard(from_right, 1).start()
    spread(from_right)
    flip_copy(0, 1, mate).wait_recv()
    flips[8] = flips[0] + flips[1]
    flip_copy(8, 2, right1).start()
    flip_copy(8, 3, left1).start()
    unpack(2 * from_left + core)
    half_shard(far, 0).wait_recv()
    half_shard(far, 1).wait_recv()
    spread(far)

    def near(i, carry):
        r1 = jnp.where(i == 0, 0, jnp.where(i == 1, 3, jnp.where(i == 2, 1, 2)))
        lower, upper = chip(core, r1, 3), chip(core, r1, 1)
        wait_shard(lower)

        @pl.when(i < 2)
        def _():
            send_shard(lower, 2)

        send_mate(lower)
        wait_shard(upper)

        @pl.when(i >= 2)
        def _():
            send_shard(upper, 3)

        send_mate(upper)
        other = chip(1 - core, r1, 0)
        wait_mate(other)

        def expand(j, c):
            unpack(jnp.where(j == 0, 2 * other + (1 - core), jnp.where(j == 1, 2 * lower + core, 2 * upper + core)))
            return c

        lax.fori_loop(0, 3, expand, 0)
        return carry

    lax.fori_loop(0, SIDE, near, 0)

    def expand_rest(j, c):
        unpack(2 * jnp.where(j == 0, from_right, far) + core)
        return c

    lax.fori_loop(0, 2, expand_rest, 0)
    flip_copy(8, 2, right1).wait_recv()
    flip_copy(2, 4, right1).start()

    def distant(i, carry):
        r1 = jnp.where(i == 0, 0, jnp.where(i == 1, 3, jnp.where(i == 2, 1, 2)))
        beyond = chip(core, r1, 2)
        wait_shard(beyond)
        send_mate(beyond)
        lower, upper = chip(1 - core, r1, 3), chip(1 - core, r1, 1)
        wait_mate(lower)
        wait_mate(upper)

        def expand(j, c):
            unpack(jnp.where(j == 0, 2 * beyond + core,
                             jnp.where(j == 1, 2 * lower + (1 - core), 2 * upper + (1 - core))))
            return c

        lax.fori_loop(0, 3, expand, 0)
        return carry

    lax.fori_loop(0, SIDE, distant, 0)

    def final(i, carry):
        r1 = jnp.where(i == 0, 0, jnp.where(i == 1, 3, jnp.where(i == 2, 1, 2)))
        b = chip(1 - core, r1, 2)
        wait_mate(b)
        unpack(2 * b + (1 - core))
        return carry

    lax.fori_loop(0, SIDE, final, 0)

    flip_copy(8, 3, left1).wait_recv()
    flip_copy(2, 4, right1).wait_recv()
    flips[9] = flips[8] + flips[2] + flips[3] + flips[4]
    flip_copy(9, 5, right2).start()
    flip_copy(9, 6, left2).start()

    def tile_rows(m):
        return pl.ds(pl.multiple_of(m * rows, rows), rows)

    def z_copy(m, c, target):
        return pltpu.make_async_remote_copy(
            src_ref=leaving.at[m, c], dst_ref=arriving.at[m, c], send_sem=z_send.at[m, c], recv_sem=z_recv.at[m, c],
            device_id={"section": target}, device_id_type=MESH)

    def forward_copy(m, c):
        return z_copy(m, c, jnp.minimum(s + 1, last))

    def backward_copy(m, c):
        return z_copy(m, c, jnp.maximum(s - 1, 0))

    def half_copy(m):
        return remote(theirs.at[tile_rows(m)], mine.at[tile_rows(m)], mate_send.at[0, m], mate_n.at[m], mate)

    def grad_copy(m):
        return remote(grad_pre.at[tile_rows(m)], grad_pre.at[tile_rows(m)], mate_send.at[0, m], mate_g.at[m], mate)

    def saved_copy(k, m):
        src = (arriving, slope, preact, scale)[k]
        dst = (hidden, slope, preact, scale)[k]
        at = m if k == 0 else tile_rows(m)
        return remote(src.at[at], dst.at[at], mate_send.at[1 + k, m], mate_f.at[k, m], mate)

    def forward(m, carry):
        at = tile_rows(m)
        squares = 0.0
        for k, deep in enumerate(pieces):
            @pl.when(s > 0)
            def _():
                forward_copy(m, k).wait_recv()

            values = arriving[m, k].astype(F32)
            gained = (values * gain_ref[:, deep]).astype(BF)
            squares += jnp.sum(values * values, axis=-1, keepdims=True)
            if k < chunks - 1:
                for cols in pieces:
                    term = jnp.dot(gained, w[deep, cols], preferred_element_type=F32)
                    partial[:, cols] = term if k == 0 else partial[:, cols] + term
        @pl.when(s == last)
        def _():
            saved_copy(0, m).start()

        q = lax.rsqrt(squares * (1.0 / width) + epsilon)
        scale[at, :] = jnp.broadcast_to(q, (rows, 128))
        for c, cols in enumerate(pieces):
            p = (partial[:, cols] + jnp.dot(gained, w[deep, cols], preferred_element_type=F32)) * q
            cdf = 0.5 * (1.0 + lax.erf(p * half_root))
            leaving[m, c] = (arriving[m, c].astype(F32) + p * cdf).astype(BF)

            @pl.when(s < last)
            def _():
                forward_copy(m, c).start()

            preact[at, cols] = p.astype(BF)
            slope[at, cols] = (cdf + p * (jnp.exp(-0.5 * p * p) * density_scale)).astype(BF)
        for k in (1, 2, 3):
            saved_copy(k, m).start()

        @pl.when(s < last)
        def _():
            saved_copy(0, m).start()

        return carry

    def halves(m, carry):
        at = tile_rows(m)
        q = scale[at, :]
        low = lax.broadcasted_iota(jnp.int32, (rows, 128), 1) < 64

        def scaled(start):
            values = arriving[m, start // chunk, :, pl.ds(start % chunk, 128)].astype(F32)
            return values * q * gain_ref[:, pl.ds(start, 128)]

        for k in range(width // 256):
            first, second = scaled(256 * k), scaled(256 * k + 128)
            cols = pl.ds(128 * k, 128)
            mine[at, cols] = jnp.where(low, pltpu.roll(first, 64, 1), second).astype(BF)
        for k in range(width // 256):
            start = (k % 2) * 1024 + (k // 2) * 128
            first, second = scaled(start), scaled(start + 512)
            theirs[at, pl.ds(128 * k, 128)] = jnp.where(low, first, pltpu.roll(second, 64, 1)).astype(BF)
        half_copy(m).start()
        return carry

    def backward(m, carry):
        at = tile_rows(m)
        for k in (1, 2):
            saved_copy(k, m).wait_recv()
        inner = 0.0
        for k, deep in enumerate(pieces):
            @pl.when(s < last)
            def _():
                backward_copy(m, k).wait_recv()

            gp = (arriving[m, k].astype(F32) * slope[at, deep].astype(F32)).astype(BF)
            grad_pre[at, deep] = gp
            inner += jnp.sum(gp.astype(F32) * preact[at, deep].astype(F32), axis=-1, keepdims=True)
            if k < chunks - 1:
                @pl.when(s > 0)
                def _():
                    for cols in pieces:
                        term = jnp.dot(gp, turned[deep, cols], preferred_element_type=F32)
                        partial[:, cols] = term if k == 0 else partial[:, cols] + term

        for k in (0, 3):
            saved_copy(k, m).wait_recv()

        @pl.when(s > 0)
        def _():
            q = scale[at, 0:1]
            pull = q * q * (inner * (1.0 / width))
            for c, cols in enumerate(pieces):
                a = partial[:, cols] + jnp.dot(gp, turned[deep, cols], preferred_element_type=F32)
                a = a * gain_ref[:, cols]
                leaving[m, c] = (arriving[m, c].astype(F32) + q * a - hidden[m, c].astype(F32) * pull).astype(BF)
                backward_copy(m, c).start()

        grad_copy(m).start()
        return carry

    def received_grad(m, carry):
        grad_copy(m).wait_recv()
        return carry

    def received_half(m, carry):
        half_copy(m).wait_recv()
        return carry

    @pl.when(forward_core)
    def _():
        @pl.when(s == 0)
        def _():
            for copy in x_copies:
                copy.wait()
            for copy in x_mates:
                copy.wait_recv()

        lax.fori_loop(0, micros, forward, 0)
        lax.fori_loop(0, micros, halves, 0)
        lax.fori_loop(0, micros, received_grad, 0)

    @pl.when(backward_core)
    def _():
        def turn(i, carry):
            at = pl.ds(pl.multiple_of(i * 128, 128), 128)
            turned[:, at] = w[at, :].T
            return carry

        lax.fori_loop(0, width // 128, turn, 0)

        @pl.when(s == last)
        def _():
            for copy in ct_copies:
                copy.wait()
            for copy in ct_mates:
                copy.wait_recv()

        lax.fori_loop(0, micros, backward, 0)
        lax.fori_loop(0, micros, received_half, 0)

    flip_copy(9, 5, right2).wait_recv()
    flip_copy(5, 7, right2).start()

    place1, place2 = jnp.where(core == 0, xx, yy), jnp.where(core == 0, yy, xx)

    def block(r1, r2):
        place = ((place1 + r1) % SIDE) * SIDE + (place2 + r2) % SIDE
        return pl.ds(pl.multiple_of(place * shard, shard), shard)

    def terms(i):
        r1 = jnp.where(i == 0, 2, jnp.where(i == 1, 3, jnp.where(i == 2, 1, 0)))
        cols = pl.ds(pl.multiple_of(((place1 + r1) % SIDE) * (SIDE * shard), SIDE * shard), SIDE * shard)
        part[cols, :] = lax.dot_general(
            mine[:, cols], grad_pre[...], (((0,), (0,)), ((), ())), preferred_element_type=F32).astype(BF)

    def slot(r2, count=1):
        return pl.ds(r2 * shard, count * shard)

    def first_ring(src_r1, r2, d, dst, dst_slot, recv):
        return remote(part.at[block(src_r1, r2)], dst.at[dst_slot], rs_send.at[d], recv, around[d])

    toward_left, toward_right = (2, 1), (3, 0)
    def group(i, carry):
        terms(i)

        @pl.when(i == 0)
        def _():
            for k in range(2):
                first_ring(2, toward_left[k], 1, part_a, slot(toward_left[k]), a_recv.at[toward_left[k]]).start()
                first_ring(2, toward_right[k], 0, part_a, slot(toward_right[k]), a_recv.at[toward_right[k]]).start()

        @pl.when(i == 1)
        def _():
            for r2 in toward_right:
                first_ring(3, r2, 1, part_b, slot(r2), ab_recv.at[0, r2]).start()

        @pl.when(i == 2)
        def _():
            for r2 in toward_left:
                first_ring(1, r2, 0, part_b, slot(4 + r2), ab_recv.at[1, r2]).start()

        return carry

    lax.fori_loop(0, SIDE, group, 0)
    def drain_forward(m, carry):
        @pl.when(s < last)
        def _():
            for c in range(chunks):
                forward_copy(m, c).wait_send()

        half_copy(m).wait_send()
        for k in range(4):
            saved_copy(k, m).wait_send()
        return carry

    def drain_backward(m, carry):
        @pl.when(s > 0)
        def _():
            for c in range(chunks):
                backward_copy(m, c).wait_send()

        grad_copy(m).wait_send()
        return carry

    @pl.when(forward_core)
    def _():
        lax.fori_loop(0, micros, drain_forward, 0)

        @pl.when(s == last)
        def _():
            for copy in ct_mates:
                copy.wait_send()

    @pl.when(backward_core)
    def _():
        lax.fori_loop(0, micros, drain_backward, 0)

        @pl.when(s == 0)
        def _():
            for copy in x_mates:
                copy.wait_send()

    def sent(sem, count):
        ref = grad_pre.at[pl.ds(0, count)]
        remote(ref, ref, sem, flip_recv.at[0], mate).wait_send()

    for d in (0, 1):
        sent(ag_send.at[d], 3 * groups)
    for d in (2, 3):
        sent(ag_send.at[d], 12 * groups)
    sent(ag_send.at[4], 2 * BLOCKS * groups)

    for k in range(2):
        for r2, r1, d, side in ((toward_left[k], 3, 1, 0), (toward_right[k], 1, 0, 1)):
            first_ring(2, r2, d, part_a, slot(r2), a_recv.at[r2]).wait_recv()
            at = block(r1, r2)
            part[at, :] = (part[at, :].astype(F32) + part_a[slot(r2), :].astype(F32)).astype(BF)
            first_ring(r1, r2, d, part_b, slot(4 * side + r2), ab_recv.at[side, r2]).start()

    flip_copy(9, 6, left2).wait_recv()
    flip_copy(5, 7, right2).wait_recv()
    all_flips = flips[9] + flips[5] + flips[6] + flips[7]
    flip_ref[0] = jnp.sum(all_flips.astype(F32)).astype(jnp.int32)

    def ring_total(r2):
        for side in range(2):
            first_ring(3, r2, 1, part_b, slot(4 * side + r2), ab_recv.at[side, r2]).wait_recv()
        total = part[block(0, r2), :].astype(F32) + part_b[slot(r2), :].astype(F32) + part_b[slot(4 + r2), :].astype(F32)
        row_sum[slot(r2), :] = total.astype(BF)

    half = shard // 2

    def second_ring(r2, h, d, dst, start, recv):
        return remote(row_sum.at[pl.ds(r2 * shard + h * half, half)], dst.at[pl.ds(start, half)], rs_send.at[d], recv,
                      around[d])

    ring_total(2)
    second_ring(2, 0, 3, row_a, 0, ra_recv.at[0]).start()
    second_ring(2, 1, 2, row_a, half, ra_recv.at[1]).start()
    ring_total(3)
    second_ring(3, 1, 3, row_b, half, rb_recv.at[0, 1]).start()
    ring_total(1)
    second_ring(1, 0, 2, row_b, shard, rb_recv.at[1, 0]).start()
    for h, r2, d, side in ((0, 3, 3, 0), (1, 1, 2, 1)):
        second_ring(2, h, d, row_a, h * half, ra_recv.at[h]).wait_recv()
        at = pl.ds(r2 * shard + h * half, half)
        row_sum[at, :] = (row_sum[at, :].astype(F32) + row_a[pl.ds(h * half, half), :].astype(F32)).astype(BF)
        second_ring(r2, h, d, row_b, side * shard + h * half, rb_recv.at[side, h]).start()
    ring_total(0)
    for side, h in ((0, 1), (1, 0), (0, 0), (1, 1)):
        second_ring(2, h, 3, row_b, side * shard + h * half, rb_recv.at[side, h]).wait_recv()
    for k in range(width // piece):
        cols = pl.ds(k * piece, piece)
        total = row_sum[slot(0), cols].astype(F32) + row_b[slot(0), cols].astype(F32) + row_b[slot(1), cols].astype(F32)
        out_ref[:, cols] = total * (1.0 / math.sqrt(token_total)) + decay[k]

    for d in (0, 1):
        sent(rs_send.at[d], 6 * shard)
    for d in (2, 3):
        sent(rs_send.at[d], 3 * half)
    for dst in range(1, 8):
        flip_copy(0, dst, mate).wait_send()


def step(x, ct, weight, gain, pair, earlier, sections, token_total, chunk):
    micros, tall, width = x.shape
    micros, rows = 2 * micros, micros * tall
    chunks = width // chunk
    shard = weight.shape[0]
    groups = shard // 4
    vmem = pl.BlockSpec(memory_space=pltpu.VMEM)
    hbm = pl.BlockSpec(memory_space=pl.ANY)
    act = pltpu.VMEM((2 * rows, width), BF)
    stream = pltpu.VMEM((micros, chunks, tall, chunk), BF)
    dma = pltpu.SemaphoreType.DMA
    return pl.pallas_call(
        functools.partial(kernel, sections, token_total),
        out_shape=(jax.ShapeDtypeStruct((shard, width), F32), jax.ShapeDtypeStruct((1,), jnp.int32)),
        in_specs=[hbm] * 6,
        out_specs=(vmem, pl.BlockSpec(memory_space=pltpu.SMEM)),
        scratch_shapes=[
            pltpu.VMEM((shard, width), BF), pltpu.VMEM((1, width), F32), pltpu.VMEM((groups, width), jnp.int32),
            pltpu.VMEM((groups, width), jnp.int32), dma((4,)),
            pltpu.VMEM((tall, width), F32),
            pltpu.VMEM((width, width), BF),
            pltpu.VMEM((width, width), BF),
            pltpu.VMEM((2 * BLOCKS, 2 * groups, width), BF),
            pltpu.VMEM(pair.shape, jnp.int32),
            pltpu.VMEM((width // 128, shard, 128), F32),
            pltpu.VMEM((width // 128, shard, 128), F32),
            stream, stream, stream, act, act, pltpu.VMEM((2 * rows, 128), F32),
            pltpu.VMEM((2 * rows, width // 2), BF),
            pltpu.VMEM((2 * rows, width // 2), BF),
            pltpu.VMEM((2 * rows, width), BF),
            pltpu.VMEM((width // 2, width), BF),
            pltpu.VMEM((SIDE * shard, width), BF),
            pltpu.VMEM((2 * SIDE * shard, width), BF),
            pltpu.VMEM((SIDE * shard, width), BF),
            pltpu.VMEM((shard, width), BF),
            pltpu.VMEM((2 * shard, width), BF),
            pltpu.VMEM((10, 8, 128), jnp.int32),
            dma((1 + chunks,)), dma((5,)), dma((BLOCKS,)), dma((2,)), dma((BLOCKS,)), dma((chunks,)), dma((chunks,)),
            dma((micros, chunks)), dma((micros, chunks)), dma((micros,)), dma((micros,)), dma((4, micros)), dma((5, micros)),
            dma((SIDE,)), dma((2, SIDE)), dma((2,)), dma((2, 2)), dma((4,)), dma((7,)), dma((7,)),
        ],
        compiler_params=pltpu.CompilerParams(
            collective_id=0, has_side_effects=True, vmem_limit_bytes=58 * 1024 * 1024),
    )(x, ct, weight, gain, pair, earlier)


def body(activations, cotangent, weight, norm_gain, pair_mask, earlier_mask):
    micro_count, row_count, model_width = activations.shape
    tokens = micro_count * row_count
    tall = 32
    gradient, flip_sum = step(
        activations.reshape(tokens // tall, tall, model_width), cotangent.reshape(tokens // tall, tall, model_width),
        weight[0], norm_gain, pair_mask[0], earlier_mask[0], lax.axis_size("section"),
        tokens * lax.axis_size("dp"), CHUNK)
    return (gradient[None], flip_sum)


def solution(mesh):
    placed = (
        P(None, "dp", None),
        P(None, "dp", None),
        P("section", "dp", None),
        P("section", None),
        P("section", None, None),
        P("section", "dp", None),
    )
    return jax.shard_map(
        body,
        mesh=mesh,
        in_specs=placed,
        out_specs=(P("section", "dp", None), P("section")),
        check_vma=False,
    )
```
